32 devices in a mesh: scen: 8 (over z, x), rootr: 2 (over core), rootc: 2 (over y).
Axes of the slice: x: 2, y: 2, z: 4, core: 2. Of those that a mesh axis runs over, the one named last changes fastest.
Arguments:
- start_guess: float32 [8192, 256], P(('scen', 'rootr'), 'rootc'), may hold values from -6 to 6
- right_side: float32 [8192, 256], P(('scen', 'rootr'), 'rootc'), may hold values from -6 to 6
- root_diagonal: float32 [8192], P(('scen', 'rootr')), may hold values from 1 to 4
- preconditioner: bfloat16 [8192, 8192], P(('scen', 'rootr')), may hold values from -0.015625 to 0.015625
- border_block: bfloat16 [16, 512, 768], P(('scen', 'rootr'), 'rootc'), may hold values from -0.21875 to 0.21875
- coupling_inverse: bfloat16 [16, 512, 512], P(('scen', 'rootr'), 'rootc'), may hold values from -0.25 to 0.25
- border_count: int32 [16], P(('scen', 'rootr')), may hold values from 64 to 512, as said below
- column_tiles: int32 [16, 6], P(('scen', 'rootr')), may hold values from 0 to 63, as said below
Outputs:
- final_iterate: float32 [8192, 256], P(('scen', 'rootr'), 'rootc')
The draws below stay inside these ranges and needn't reach their ends.
Inputs may be any that keep to these rules, and one draw needn't show every extreme that they name: A scenario's live border rows are its first border_count rows; some scenario has exactly 512. `column_tiles`: each row names 6 different tiles in rising order.
All inputs are finite; a program needn't handle non-finite values.
Results may differ from the reference program's by a relative error of at most 0.0022.
Values may be sent and summed in bfloat16 or wider, within the bound.
A program may use at most 64 MiB of HBM per device.

```python
import math
import jax
import jax.numpy as jnp
from jax import lax

ORDER = 8192
RHS = 256
BORDER = 512
TILE = 128
TOUCHED = 6
ITERS = 1
SCEN = 16
NTILES = 64
COUPLED = 768


def draw_border_count(key, part):
    first_key, second_key = jax.random.split(key)
    divisor = jax.random.randint(first_key, (SCEN,), 1, 9)
    counts = BORDER // divisor
    chosen = jax.random.randint(second_key, (), 0, SCEN)
    return jnp.where(jnp.arange(SCEN) == chosen, BORDER, counts).astype(jnp.int32)


def draw_column_tiles(key, part):
    scores = jax.random.randint(key, (SCEN, NTILES), 0, 1 << 20) * NTILES + jnp.arange(NTILES)[None, :]
    ordering = jnp.argsort(scores, axis=1)[:, :TOUCHED]
    return jnp.sort(ordering, axis=1).astype(jnp.int32)


def shard_levels(key, extent, pieces, least, largest):
    loudness, own = 1.0, jax.random.fold_in(key, 6)
    for position, parts in pieces:
        draws = jnp.exp(jax.random.uniform(jax.random.fold_in(own, position), (parts,), jnp.float32, least / len(pieces), largest / len(pieces)))
        loudness = loudness * jnp.repeat(draws, extent[position] // parts).reshape([-1 if axis == position else 1 for axis in range(len(extent))])
    return loudness


def centred(rng, extent, width, most, pieces=(), dtype=jnp.bfloat16):
    loudness = shard_levels(rng, extent, pieces, -0.22, 0.18) if pieces else 1.0
    values = jax.random.normal(rng, extent, jnp.float32) * width * loudness
    return jnp.minimum(jnp.maximum(values, -most), most).astype(dtype)


def setup_inputs(seed: int = 0) -> dict:
    seeds = jax.random.split(jax.random.key(seed), 9)
    start_guess = centred(seeds[0], (ORDER, RHS), 1.0, 6.0, ((0, 16), (1, 2)), jnp.float32)
    right_side = centred(seeds[1], (ORDER, RHS), 1.0, 6.0, ((0, 16), (1, 2)), jnp.float32)
    root_diagonal = jnp.clip(jnp.exp(math.log(4.0) - 1.3862944 * jax.random.uniform(seeds[2], (ORDER,), jnp.float32) ** shard_levels(seeds[2], (ORDER,), ((0, 16),), -0.2, 0.2)), 1.0, 4.0)
    preconditioner = centred(seeds[3], (ORDER, ORDER), (16 * ORDER) ** -0.5, 0.015625, ((0, 16),))
    border_block = centred(seeds[4], (SCEN, BORDER, COUPLED), COUPLED ** -0.5, 0.21875, ((0, 16), (1, 2)))
    coupling_inverse = centred(seeds[5], (SCEN, BORDER, BORDER), BORDER ** -0.5, 0.25, ((0, 16), (1, 2)))
    border_count = draw_border_count(jax.random.fold_in(seeds[8], 71), 0)
    column_tiles = draw_column_tiles(jax.random.fold_in(seeds[8], 71), 0)
    return {"start_guess": start_guess, "right_side": right_side, "root_diagonal": root_diagonal, "preconditioner": preconditioner, "border_block": border_block, "coupling_inverse": coupling_inverse, "border_count": border_count, "column_tiles": column_tiles}


def scenario_term(iterate_low, border, inverse_rows, live_count, tile_ids):
    picked = iterate_low.reshape(NTILES, TILE, RHS)[tile_ids].reshape(COUPLED, RHS)
    live_rows = (jnp.arange(BORDER) < live_count)[:, None]
    border_values = jnp.dot(border, picked, preferred_element_type=jnp.float32)
    border_values = jnp.where(live_rows, border_values, 0.0).astype(jnp.bfloat16)
    solved = jnp.dot(inverse_rows, border_values, preferred_element_type=jnp.float32)
    solved = jnp.where(live_rows, solved, 0.0).astype(jnp.bfloat16)
    return jnp.dot(border.T, solved, preferred_element_type=jnp.float32)


def reference(start_guess, right_side, root_diagonal, preconditioner, border_block, coupling_inverse, border_count, column_tiles):
    iterate = start_guess
    for iteration in range(ITERS):
        iterate_low = iterate.astype(jnp.bfloat16)

        def accumulate(running, scenario):
            border, inverse_rows, live_count, tile_ids = scenario
            term = scenario_term(iterate_low, border, inverse_rows, live_count, tile_ids)
            running = running.reshape(NTILES, TILE, RHS).at[tile_ids].add(term.reshape(TOUCHED, TILE, RHS))
            return running.reshape(ORDER, RHS), None

        coupling, unused = lax.scan(accumulate, jnp.zeros((ORDER, RHS), jnp.float32), (border_block, coupling_inverse, border_count, column_tiles))
        residual = right_side - root_diagonal[:, None] * iterate + coupling
        iterate = iterate + jnp.dot(preconditioner, residual.astype(jnp.bfloat16), preferred_element_type=jnp.float32)
    return iterate
```

```python
import functools
import math

import jax
import jax.numpy as jnp
from jax import lax
from jax.experimental import pallas as pl
from jax.experimental.pallas import tpu as pltpu
from jax.sharding import PartitionSpec as P

TILE = 128
MESH = pl.DeviceIdType.MESH
LOW_STEP = 1
OWN_STEP = 1
TERM_STEP = 1
EARLY = 2


class Place:
    def __init__(self, count):
        self.count, self.hops = count, count // 2
        self.scen, self.core = lax.axis_index("scen"), lax.axis_index("rootr")
        side, level = lax.rem(self.scen, 2), lax.div(self.scen, 2)
        self.spot = level * (1 - side) + (count - 1 - level) * side
        self.ahead = [self.at(1), self.at(count - 1)]

    def at(self, shift):
        spot = lax.rem(self.spot + shift, self.count)
        upper = lax.div(spot, self.hops)
        return (1 - upper) * 2 * spot + upper * (2 * (self.count - 1 - spot) + 1)

    def origin(self, way, hop):
        return self.at(self.count - hop if way == 0 else hop)

    def origins(self, hop):
        if hop == 0:
            return [self.scen]
        if hop == self.hops:
            return [self.origin(0, hop)]
        return [self.origin(0, hop), self.origin(1, hop)]


class Stream:
    def __init__(self, place, buf, rows, step, sems):
        self.place, self.buf, self.rows, self.step = place, buf, rows, step
        self.chunks = rows // step
        self.ring_send, self.ring_recv, self.pair_send, self.pair_recv = sems
        self.ring_rows = self.pair_rows = 0

    def piece(self, scen, core, chunk):
        first = (scen * 2 + core) * self.rows + chunk * self.step
        return self.buf.at[pl.ds(first, self.step)]

    def carried(self, way, hop):
        if hop < self.place.hops:
            return range(self.chunks)
        half = (self.chunks + 1) // 2
        return range(half) if way == 0 else range(half, self.chunks)

    def rounds(self, hop, chunks=None):
        chunks = range(self.chunks) if chunks is None else chunks
        ways = [[(way, c) for c in self.carried(way, hop) if c in chunks] for way in range(2)]
        return [
            [way[i] for way in ways if i < len(way)] for i in range(max(len(way) for way in ways))
        ]

    def ring_copy(self, way, hop, chunk, scen):
        ref = self.piece(scen, self.place.core, chunk)
        return pltpu.make_async_remote_copy(
            src_ref=ref,
            dst_ref=ref,
            send_sem=self.ring_send.at[0],
            recv_sem=self.ring_recv.at[(way * self.place.hops + hop - 1) * self.chunks + chunk],
            device_id={"scen": self.place.ahead[way]},
            device_id_type=MESH,
        )

    def pair_copy(self, hop, ref):
        return pltpu.make_async_remote_copy(
            src_ref=ref,
            dst_ref=ref,
            send_sem=self.pair_send.at[0],
            recv_sem=self.pair_recv.at[hop],
            device_id={"rootr": 1 - self.place.core},
            device_id_type=MESH,
        )

    def send(self, way, hop, chunk, scen):
        if chunk in self.carried(way, hop):
            self.ring_copy(way, hop, chunk, scen).start()
            self.ring_rows += self.step

    def share(self, hop, chunk, scen):
        self.pair_copy(hop, self.piece(scen, self.place.core, chunk)).start()
        self.pair_rows += self.step

    def begin(self, chunks=None):
        for chunk in range(self.chunks) if chunks is None else chunks:
            for way in range(2):
                self.send(way, 1, chunk, self.place.scen)

    def begin_share(self):
        for chunk in range(self.chunks):
            self.share(0, chunk, self.place.scen)

    def arrive(self, hop, arrivals):
        for way, chunk in arrivals:
            scen = self.place.origin(way, hop)
            self.ring_copy(way, hop, chunk, scen).wait_recv()
            if hop < self.place.hops:
                self.send(way, hop + 1, chunk, scen)
            self.share(hop, chunk, scen)

    def settle(self, hop):
        whole = self.rows if hop in (0, self.place.hops) else 2 * self.rows
        self.pair_copy(hop, self.buf.at[pl.ds(0, whole)]).wait_recv()

    def finish(self):
        ref = self.buf.at[pl.ds(0, self.ring_rows)]
        pltpu.make_async_remote_copy(
            src_ref=ref,
            dst_ref=ref,
            send_sem=self.ring_send.at[0],
            recv_sem=self.ring_recv.at[0],
            device_id={"scen": self.place.ahead[0]},
            device_id_type=MESH,
        ).wait_send()
        self.pair_copy(0, self.buf.at[pl.ds(0, self.pair_rows)]).wait_send()


def kernel(
    count,
    guess_hbm,
    right_hbm,
    diagonal_hbm,
    precon_hbm,
    border_hbm,
    inverse_hbm,
    live_ref,
    own_tiles_ref,
    out_ref,
    guess,
    right,
    diagonal,
    low_all,
    own_all,
    term_all,
    tiles_all,
    tiles_smem,
    precon,
    border,
    inverse,
    local_sems,
    cross_send,
    cross_recv,
    *ring_sems,
):
    place = Place(count)
    hops = place.hops
    side = lax.axis_index("rootc")
    own_rows, half_rhs = guess.shape
    half_rows, coupled = border_hbm.shape[1:]
    touched = coupled // TILE
    own_block = place.scen * 2 + place.core

    barrier = pltpu.get_barrier_semaphore()
    peers = (
        {"scen": place.ahead[0]},
        {"scen": place.ahead[1]},
        {"rootr": 1 - place.core},
        {"rootc": 1 - side},
    )
    for peer in peers:
        pl.semaphore_signal(barrier, inc=1, device_id=peer, device_id_type=MESH)

    load_guess = pltpu.make_async_copy(guess_hbm, guess, local_sems.at[0])
    load_right = pltpu.make_async_copy(right_hbm, right, local_sems.at[1])
    load_diagonal = pltpu.make_async_copy(diagonal_hbm, diagonal, local_sems.at[2])
    own_half = pl.ds(pl.multiple_of(side * half_rows, half_rows), half_rows)
    load_border = pltpu.make_async_copy(border_hbm.at[0], border.at[own_half], local_sems.at[3])
    load_inverse = pltpu.make_async_copy(inverse_hbm.at[0], inverse.at[own_half], local_sems.at[4])
    columns_count = precon.shape[0]
    for load in (load_guess, load_right, load_diagonal, load_border, load_inverse):
        load.start()

    unit = low_all.shape[1]
    units = own_rows // unit
    per_tile = TILE // unit
    own_slice = pl.ds(own_block * units, units)
    split = (units, unit, half_rhs)
    lanes = lax.broadcasted_iota(jnp.int32, (1, 1, TILE), 2)
    tiles_row = jnp.zeros((1, 1, TILE), jnp.int32)
    for k in range(touched):
        tiles_row = jnp.where(lanes == k, own_tiles_ref[0, k], tiles_row)
    tiles_all[pl.ds(own_block, 1)] = tiles_row
    load_guess.wait()
    low_all[own_slice] = guess[...].astype(jnp.bfloat16).reshape(split)

    low = Stream(place, low_all, units, min(LOW_STEP, units), ring_sems[0:4])
    own = Stream(place, own_all, units, min(OWN_STEP, units), ring_sems[4:8])
    term = Stream(place, term_all, touched, TERM_STEP, ring_sems[8:12])
    tiles = Stream(place, tiles_all, 1, 1, ring_sems[12:16])
    early = range(min(EARLY, own.chunks))
    late = range(len(early), own.chunks)

    pl.semaphore_wait(barrier, len(peers))
    low.begin()
    crossings = []
    for index, (source, target) in enumerate(((border_hbm, border), (inverse_hbm, inverse))):
        crossing = pltpu.make_async_remote_copy(
            src_ref=source.at[0],
            dst_ref=target.at[own_half],
            send_sem=cross_send.at[index],
            recv_sem=cross_recv.at[index],
            device_id={"rootc": 1 - side},
            device_id_type=MESH,
        )
        crossing.start()
        crossings.append(crossing)
    low.begin_share()
    tiles.begin()

    load_right.wait()
    load_diagonal.wait()
    scale = jnp.broadcast_to(diagonal[...], (half_rhs, own_rows)).T
    own_terms = right[...] - scale * guess[...]
    own_all[own_slice] = own_terms.astype(jnp.bfloat16).reshape(split)
    own.begin(early)
    own.begin_share()
    tiles.begin_share()

    @pl.loop(0, columns_count)
    def start_column(t):
        columns = pl.ds(pl.multiple_of(t * TILE, TILE), TILE)
        pltpu.make_async_copy(precon_hbm.at[:, columns], precon.at[t], local_sems.at[5]).start()

    for hop in range(1, hops + 1):
        for arrivals in low.rounds(hop):
            low.arrive(hop, arrivals)
        for arrivals in tiles.rounds(hop):
            tiles.arrive(hop, arrivals)
        if hop == hops - 1:
            own.begin(late)
        if hop == hops:
            for arrivals in own.rounds(1, late):
                own.arrive(1, arrivals)
        for arrivals in own.rounds(hop, early):
            own.arrive(hop, arrivals)
    for hop in range(hops + 1):
        low.settle(hop)

    load_border.wait()
    crossings[0].wait_recv()
    live = jnp.clip(live_ref[0], 0, 2 * half_rows)
    live_mask = lax.broadcasted_iota(jnp.int32, (2 * half_rows, half_rhs), 0) < live
    picked = jnp.concatenate(
        [
            low_all[own_tiles_ref[0, k] * per_tile + part]
            for k in range(touched)
            for part in range(per_tile)
        ],
        axis=0,
    )
    values = jnp.dot(border[...], picked, preferred_element_type=jnp.float32)
    values = jnp.where(live_mask, values, 0.0).astype(jnp.bfloat16)
    load_inverse.wait()
    crossings[1].wait_recv()
    solved = jnp.dot(inverse[...], values, preferred_element_type=jnp.float32)
    solved = jnp.where(live_mask, solved, 0.0).astype(jnp.bfloat16)
    terms = lax.dot_general(
        border[...], solved, (((0,), (0,)), ((), ())), preferred_element_type=jnp.float32
    )
    term_all[pl.ds(own_block * touched, touched)] = terms.astype(jnp.bfloat16).reshape(
        touched, TILE, half_rhs
    )
    term.begin()
    term.begin_share()

    for hop in range(hops + 1):
        tiles.settle(hop)
    to_smem = pltpu.make_async_copy(tiles_all, tiles_smem, local_sems.at[6])
    to_smem.start()
    pltpu.make_async_copy(precon, precon, local_sems.at[5]).wait()
    out_ref[...] = guess[...]
    to_smem.wait()

    def product(columns, values, rows):
        left = jnp.concatenate([precon[t] for t in columns], axis=1)
        right = jnp.concatenate([values[t] for t in rows], axis=0)
        return jnp.dot(left, right, preferred_element_type=jnp.float32)

    own_tiles = own_rows // TILE

    def add_own(block):
        total = jnp.zeros_like(out_ref)
        for k in range(0, own_tiles, 2):
            group = [block * own_tiles + j for j in range(k, min(k + 2, own_tiles))]
            total = total + product(group, own_all, group)
        out_ref[...] += total

    def add_term(block):
        total = jnp.zeros_like(out_ref)
        for k in range(0, touched, 2):
            group = range(k, min(k + 2, touched))
            total = total + product(
                [tiles_smem[block, 0, j] for j in group],
                term_all,
                [block * touched + j for j in group],
            )
        out_ref[...] += total

    def work(stream, add, hop):
        blocks = [scen * 2 + core for core in range(2) for scen in place.origins(hop)]
        return [lambda: stream.settle(hop)] + [functools.partial(add, block) for block in blocks]

    def run(todo, count):
        for _ in range(min(count, len(todo))):
            todo.pop(0)()

    whole_tiles = own_rows % TILE == 0
    todo = work(own, add_own, 0) if whole_tiles else []
    for hop in range(1, hops + 1):
        todo += work(term, add_term, hop - 1)
        own_rounds = own.rounds(hop + 1, late) if hop < hops and late else []
        rounds = term.rounds(hop)
        if whole_tiles:
            todo += work(own, add_own, hop)
        share = -(-len(todo) // len(rounds))
        for arrivals in rounds:
            term.arrive(hop, arrivals)
            if own_rounds:
                own.arrive(hop + 1, own_rounds.pop(0))
            run(todo, share)
        for arrivals in own_rounds:
            own.arrive(hop + 1, arrivals)
        run(todo, len(todo))
    todo = work(term, add_term, hops)
    run(todo, len(todo))
    if not whole_tiles:
        for hop in range(hops + 1):
            own.settle(hop)

        @pl.loop(0, columns_count)
        def add_column(t):
            rows = [t * per_tile + part for part in range(per_tile)]
            out_ref[...] += product([t], own_all, rows)

    for stream in (low, own, term, tiles):
        stream.finish()
    for crossing in crossings:
        crossing.wait_send()


def local(
    count,
    start_guess,
    right_side,
    root_diagonal,
    preconditioner,
    border_block,
    coupling_inverse,
    border_count,
    column_tiles,
):
    own_rows, half_rhs = start_guess.shape
    order = preconditioner.shape[1]
    half_rows, coupled = border_block.shape[1:]
    blocks = count * 2
    touched = column_tiles.shape[1]
    hops = count // 2
    ring_sems = []
    unit = math.gcd(own_rows, TILE)
    units = own_rows // unit
    for rows, step in ((units, LOW_STEP), (units, OWN_STEP), (touched, TERM_STEP), (1, 1)):
        chunks = rows // min(step, rows)
        ring_sems += [
            pltpu.SemaphoreType.DMA((1,)),
            pltpu.SemaphoreType.DMA((2 * hops * chunks,)),
            pltpu.SemaphoreType.DMA((1,)),
            pltpu.SemaphoreType.DMA((hops + 1,)),
        ]
    vmem = pl.BlockSpec(memory_space=pltpu.VMEM)
    smem = pl.BlockSpec(memory_space=pltpu.SMEM)
    anywhere = pl.BlockSpec(memory_space=pltpu.HBM)
    return pl.pallas_call(
        functools.partial(kernel, count),
        out_shape=jax.ShapeDtypeStruct((own_rows, half_rhs), jnp.float32),
        in_specs=[anywhere] * 6 + [smem, smem],
        out_specs=vmem,
        scratch_shapes=[
            pltpu.VMEM((own_rows, half_rhs), jnp.float32),
            pltpu.VMEM((own_rows, half_rhs), jnp.float32),
            pltpu.VMEM((1, own_rows), jnp.float32),
            pltpu.VMEM((order // unit, unit, half_rhs), jnp.bfloat16),
            pltpu.VMEM((order // unit, unit, half_rhs), jnp.bfloat16),
            pltpu.VMEM((blocks * touched, TILE, half_rhs), jnp.bfloat16),
            pltpu.VMEM((blocks, 1, TILE), jnp.int32),
            pltpu.SMEM((blocks, 1, TILE), jnp.int32),
            pltpu.VMEM((order // TILE, own_rows, TILE), jnp.bfloat16),
            pltpu.VMEM((2 * half_rows, coupled), jnp.bfloat16),
            pltpu.VMEM((2 * half_rows, 2 * half_rows), jnp.bfloat16),
            pltpu.SemaphoreType.DMA((7,)),
            pltpu.SemaphoreType.DMA((2,)),
            pltpu.SemaphoreType.DMA((2,)),
        ]
        + ring_sems,
        compiler_params=pltpu.CompilerParams(
            collective_id=0, has_side_effects=True, vmem_limit_bytes=60 * 1024 * 1024
        ),
    )(
        start_guess,
        right_side,
        root_diagonal[None, :],
        preconditioner,
        border_block,
        coupling_inverse,
        border_count,
        column_tiles,
    )


def solution(mesh):
    rows = ("scen", "rootr")
    placed = (
        P(rows, "rootc"),
        P(rows, "rootc"),
        P(rows),
        P(rows, None),
        P(rows, "rootc", None),
        P(rows, "rootc", None),
        P(rows),
        P(rows, None),
    )
    return jax.shard_map(
        functools.partial(local, mesh.shape["scen"]),
        mesh=mesh,
        in_specs=placed,
        out_specs=P(rows, "rootc"),
        check_vma=False,
    )
```

```python
import functools
import math

import jax
import jax.numpy as jnp
from jax import lax
from jax.experimental import pallas as pl
from jax.experimental.pallas import tpu as pltpu
from jax.sharding import PartitionSpec as P

TILE = 128
MESH = pl.DeviceIdType.MESH
LOW_STEP = 1
OWN_STEP = 2
TERM_STEP = 2
AHEAD = 2


class Place:
    def __init__(self, count):
        self.count, self.hops = count, count // 2
        self.scen, self.core = lax.axis_index("scen"), lax.axis_index("rootr")
        side, level = lax.rem(self.scen, 2), lax.div(self.scen, 2)
        self.spot = level * (1 - side) + (count - 1 - level) * side
        self.ahead = [self.at(1), self.at(count - 1)]

    def at(self, shift):
        spot = lax.rem(self.spot + shift, self.count)
        upper = lax.div(spot, self.hops)
        return (1 - upper) * 2 * spot + upper * (2 * (self.count - 1 - spot) + 1)

    def origin(self, way, hop):
        return self.at(self.count - hop if way == 0 else hop)

    def origins(self, hop):
        if hop == 0:
            return [self.scen]
        if hop == self.hops:
            return [self.origin(0, hop)]
        return [self.origin(0, hop), self.origin(1, hop)]


class Stream:
    def __init__(self, place, hub, buf, rows, step, sems):
        self.hub = hub
        self.place, self.buf, self.rows, self.step = place, buf, rows, step
        self.chunks = rows // step
        self.ring_send, self.ring_recv, self.pair_send, self.pair_recv = sems
        self.forwarded = self.shared = 0

    def piece(self, scen, core, chunk):
        first = (scen * 2 + core) * self.rows + chunk * self.step
        return self.buf.at[pl.ds(first, self.step)]

    def carried(self, way, hop, core):
        return hop < self.place.hops or way == core

    def rounds(self, hop):
        return [
            [
                (way, core, chunk)
                for core in (self.hub, 1 - self.hub)
                for way in range(2)
                if self.carried(way, hop, core)
            ]
            for chunk in range(self.chunks)
        ]

    def ring_copy(self, way, hop, core, chunk, ref):
        slot = ((way * self.place.hops + hop - 1) * 2 + core) * self.chunks + chunk
        return pltpu.make_async_remote_copy(
            src_ref=ref,
            dst_ref=ref,
            send_sem=self.ring_send.at[0],
            recv_sem=self.ring_recv.at[slot],
            device_id={"scen": self.place.ahead[way], "rootr": self.hub},
            device_id_type=MESH,
        )

    def pair_copy(self, hop, ref):
        return pltpu.make_async_remote_copy(
            src_ref=ref,
            dst_ref=ref,
            send_sem=self.pair_send.at[0],
            recv_sem=self.pair_recv.at[hop],
            device_id={"rootr": 1 - self.place.core},
            device_id_type=MESH,
        )

    def begin(self):
        for core in range(2):

            @pl.when(self.place.core == core)
            def send():
                for chunk in range(self.chunks):
                    ref = self.piece(self.place.scen, core, chunk)
                    for way in range(2):
                        if self.carried(way, 1, core):
                            self.ring_copy(way, 1, core, chunk, ref).start()

        own = self.buf.at[pl.ds((self.place.scen * 2 + self.place.core) * self.rows, self.rows)]
        self.pair_copy(0, own).start()

    def relay(self, hop, arrivals):
        for way, core, chunk in arrivals:
            self.forwarded += self.step * (hop < self.place.hops and self.carried(way, hop + 1, core))
            self.shared += self.step

        @pl.when(self.place.core == self.hub)
        def forward():
            for way, core, chunk in arrivals:
                ref = self.piece(self.place.origin(way, hop), core, chunk)
                self.ring_copy(way, hop, core, chunk, ref).wait_recv()
                if hop < self.place.hops and self.carried(way, hop + 1, core):
                    self.ring_copy(way, hop + 1, core, chunk, ref).start()
                self.pair_copy(hop, ref).start()

    def settle(self, hop):
        if hop == 0:
            self.pair_copy(0, self.buf.at[pl.ds(0, self.rows)]).wait_recv()
            return

        @pl.when(self.place.core != self.hub)
        def arrived():
            rows = (2 if hop == self.place.hops else 4) * self.rows
            self.pair_copy(hop, self.buf.at[pl.ds(0, rows)]).wait_recv()

    def finish(self):
        for core in range(2):
            ways = sum(self.carried(way, 1, core) for way in range(2))
            ring_rows = ways * self.rows + (core == self.hub) * self.forwarded
            pair_rows = self.rows + (core == self.hub) * self.shared

            @pl.when(self.place.core == core)
            def sent():
                ref = self.buf.at[pl.ds(0, ring_rows)]
                self.ring_copy(0, 1, 0, 0, ref).wait_send()
                self.pair_copy(0, self.buf.at[pl.ds(0, pair_rows)]).wait_send()


def kernel(
    count,
    guess_hbm,
    right_hbm,
    diagonal_hbm,
    precon_hbm,
    border_hbm,
    inverse_hbm,
    live_ref,
    own_tiles_ref,
    out_ref,
    guess,
    right,
    diagonal,
    low_all,
    own_all,
    term_all,
    tiles_all,
    tiles_smem,
    precon,
    border,
    inverse,
    local_sems,
    cross_send,
    cross_recv,
    *ring_sems,
):
    place = Place(count)
    hops = place.hops
    side = lax.axis_index("rootc")
    own_rows, half_rhs = guess.shape
    half_rows, coupled = border_hbm.shape[1:]
    touched = coupled // TILE
    own_block = place.scen * 2 + place.core

    barrier = pltpu.get_barrier_semaphore()
    peers = [{"scen": scen, "rootr": core} for scen in place.ahead for core in range(2)]
    peers += [{"rootr": 1 - place.core}, {"rootc": 1 - side}]
    for peer in peers:
        pl.semaphore_signal(barrier, inc=1, device_id=peer, device_id_type=MESH)

    load_guess = pltpu.make_async_copy(guess_hbm, guess, local_sems.at[0])
    load_right = pltpu.make_async_copy(right_hbm, right, local_sems.at[1])
    load_diagonal = pltpu.make_async_copy(diagonal_hbm, diagonal, local_sems.at[2])
    own_half = pl.ds(pl.multiple_of(side * half_rows, half_rows), half_rows)
    load_border = pltpu.make_async_copy(border_hbm.at[0], border.at[own_half], local_sems.at[3])
    load_inverse = pltpu.make_async_copy(inverse_hbm.at[0], inverse.at[own_half], local_sems.at[4])
    columns_count = precon.shape[0]
    for load in (load_guess, load_right, load_diagonal, load_border, load_inverse):
        load.start()

    unit = low_all.shape[1]
    units = own_rows // unit
    per_tile = TILE // unit
    own_slice = pl.ds(own_block * units, units)
    split = (units, unit, half_rhs)
    lanes = lax.broadcasted_iota(jnp.int32, (1, 1, TILE), 2)
    tiles_row = jnp.zeros((1, 1, TILE), jnp.int32)
    for k in range(touched):
        tiles_row = jnp.where(lanes == k, own_tiles_ref[0, k], tiles_row)
    tiles_all[pl.ds(own_block, 1)] = tiles_row
    load_guess.wait()
    low_all[own_slice] = guess[...].astype(jnp.bfloat16).reshape(split)

    low = Stream(place, 1, low_all, units, min(LOW_STEP, units), ring_sems[0:4])
    own = Stream(place, 0, own_all, units, min(OWN_STEP, units), ring_sems[4:8])
    term = Stream(place, 1, term_all, touched, TERM_STEP, ring_sems[8:12])
    tiles = Stream(place, 1, tiles_all, 1, 1, ring_sems[12:16])

    pl.semaphore_wait(barrier, len(peers))
    low.begin()
    crossings = []
    for index, (source, target) in enumerate(((border_hbm, border), (inverse_hbm, inverse))):
        crossing = pltpu.make_async_remote_copy(
            src_ref=source.at[0],
            dst_ref=target.at[own_half],
            send_sem=cross_send.at[index],
            recv_sem=cross_recv.at[index],
            device_id={"rootc": 1 - side},
            device_id_type=MESH,
        )
        crossing.start()
        crossings.append(crossing)
    tiles.begin()

    load_right.wait()
    load_diagonal.wait()
    scale = jnp.broadcast_to(diagonal[...], (half_rhs, own_rows)).T
    own_terms = right[...] - scale * guess[...]
    own_all[own_slice] = own_terms.astype(jnp.bfloat16).reshape(split)

    @pl.loop(0, columns_count)
    def start_column(t):
        columns = pl.ds(pl.multiple_of(t * TILE, TILE), TILE)
        pltpu.make_async_copy(precon_hbm.at[:, columns], precon.at[t], local_sems.at[5]).start()

    for hop in range(1, hops + 1):
        for arrivals in low.rounds(hop):
            low.relay(hop, arrivals)
        if hop == max(hops - AHEAD, 1):
            low.settle(hop)
            own.begin()
        for arrivals in tiles.rounds(hop):
            tiles.relay(hop, arrivals)
    flow = [(hop, arrivals) for hop in range(1, hops + 1) for arrivals in own.rounds(hop)]

    def drain(stop):
        while flow and flow[0][0] <= stop:
            own.relay(*flow.pop(0))

    drain(1)
    for hop in range(hops + 1):
        if hop != max(hops - AHEAD, 1):
            low.settle(hop)

    load_border.wait()
    crossings[0].wait_recv()
    live = jnp.clip(live_ref[0], 0, 2 * half_rows)
    live_mask = lax.broadcasted_iota(jnp.int32, (2 * half_rows, half_rhs), 0) < live
    picked = jnp.concatenate(
        [
            low_all[own_tiles_ref[0, k] * per_tile + part]
            for k in range(touched)
            for part in range(per_tile)
        ],
        axis=0,
    )
    values = jnp.dot(border[...], picked, preferred_element_type=jnp.float32)
    values = jnp.where(live_mask, values, 0.0).astype(jnp.bfloat16)
    drain(2)
    load_inverse.wait()
    crossings[1].wait_recv()
    solved = jnp.dot(inverse[...], values, preferred_element_type=jnp.float32)
    solved = jnp.where(live_mask, solved, 0.0).astype(jnp.bfloat16)
    terms = lax.dot_general(
        border[...], solved, (((0,), (0,)), ((), ())), preferred_element_type=jnp.float32
    )
    term_all[pl.ds(own_block * touched, touched)] = terms.astype(jnp.bfloat16).reshape(
        touched, TILE, half_rhs
    )
    term.begin()

    for hop in range(hops + 1):
        tiles.settle(hop)
    to_smem = pltpu.make_async_copy(tiles_all, tiles_smem, local_sems.at[6])
    to_smem.start()
    pltpu.make_async_copy(precon, precon, local_sems.at[5]).wait()
    out_ref[...] = guess[...]
    to_smem.wait()

    def product(columns, values, rows):
        left = jnp.concatenate([precon[t] for t in columns], axis=1)
        right = jnp.concatenate([values[t] for t in rows], axis=0)
        return jnp.dot(left, right, preferred_element_type=jnp.float32)

    own_tiles = own_rows // TILE

    def add_own(block):
        total = jnp.zeros_like(out_ref)
        for k in range(0, own_tiles, 2):
            group = [block * own_tiles + j for j in range(k, min(k + 2, own_tiles))]
            total = total + product(group, own_all, group)
        out_ref[...] += total

    def add_term(block):
        total = jnp.zeros_like(out_ref)
        for k in range(0, touched, 2):
            group = range(k, min(k + 2, touched))
            total = total + product(
                [tiles_smem[block, 0, j] for j in group],
                term_all,
                [block * touched + j for j in group],
            )
        out_ref[...] += total

    def work(stream, add, hop):
        blocks = [scen * 2 + core for core in range(2) for scen in place.origins(hop)]
        return [lambda: stream.settle(hop)] + [functools.partial(add, block) for block in blocks]

    def run(todo, count):
        for _ in range(min(count, len(todo))):
            todo.pop(0)()

    whole_tiles = own_rows % TILE == 0
    todo = work(own, add_own, 0) if whole_tiles else []
    for hop in range(1, hops + 1):
        todo += work(term, add_term, hop - 1)
        if whole_tiles:
            todo += work(own, add_own, hop)
        rounds = term.rounds(hop)
        share = -(-len(todo) // len(rounds))
        for arrivals in rounds:
            if flow:
                own.relay(*flow.pop(0))
            term.relay(hop, arrivals)
            if flow and flow[0][0] <= hop:
                own.relay(*flow.pop(0))
            run(todo, share)
        drain(hop + 1)
        run(todo, len(todo))
    todo = work(term, add_term, hops)
    run(todo, len(todo))
    if not whole_tiles:
        for hop in range(hops + 1):
            own.settle(hop)

        @pl.loop(0, columns_count)
        def add_column(t):
            rows = [t * per_tile + part for part in range(per_tile)]
            out_ref[...] += product([t], own_all, rows)

    drain(hops)
    for stream in (low, own, term, tiles):
        stream.finish()
    for crossing in crossings:
        crossing.wait_send()


def local(
    count,
    start_guess,
    right_side,
    root_diagonal,
    preconditioner,
    border_block,
    coupling_inverse,
    border_count,
    column_tiles,
):
    own_rows, half_rhs = start_guess.shape
    order = preconditioner.shape[1]
    half_rows, coupled = border_block.shape[1:]
    blocks = count * 2
    touched = column_tiles.shape[1]
    hops = count // 2
    ring_sems = []
    unit = math.gcd(own_rows, TILE)
    units = own_rows // unit
    for rows, step in ((units, LOW_STEP), (units, OWN_STEP), (touched, TERM_STEP), (1, 1)):
        chunks = rows // min(step, rows)
        ring_sems += [
            pltpu.SemaphoreType.DMA((1,)),
            pltpu.SemaphoreType.DMA((4 * hops * chunks,)),
            pltpu.SemaphoreType.DMA((1,)),
            pltpu.SemaphoreType.DMA((hops + 1,)),
        ]
    vmem = pl.BlockSpec(memory_space=pltpu.VMEM)
    smem = pl.BlockSpec(memory_space=pltpu.SMEM)
    anywhere = pl.BlockSpec(memory_space=pltpu.HBM)
    return pl.pallas_call(
        functools.partial(kernel, count),
        out_shape=pltpu.VMEM((own_rows, half_rhs), jnp.float32),
        in_specs=[anywhere] * 6 + [smem, smem],
        out_specs=vmem,
        scratch_shapes=[
            pltpu.VMEM((own_rows, half_rhs), jnp.float32),
            pltpu.VMEM((own_rows, half_rhs), jnp.float32),
            pltpu.VMEM((1, own_rows), jnp.float32),
            pltpu.VMEM((order // unit, unit, half_rhs), jnp.bfloat16),
            pltpu.VMEM((order // unit, unit, half_rhs), jnp.bfloat16),
            pltpu.VMEM((blocks * touched, TILE, half_rhs), jnp.bfloat16),
            pltpu.VMEM((blocks, 1, TILE), jnp.int32),
            pltpu.SMEM((blocks, 1, TILE), jnp.int32),
            pltpu.VMEM((order // TILE, own_rows, TILE), jnp.bfloat16),
            pltpu.VMEM((2 * half_rows, coupled), jnp.bfloat16),
            pltpu.VMEM((2 * half_rows, 2 * half_rows), jnp.bfloat16),
            pltpu.SemaphoreType.DMA((7,)),
            pltpu.SemaphoreType.DMA((2,)),
            pltpu.SemaphoreType.DMA((2,)),
        ]
        + ring_sems,
        compiler_params=pltpu.CompilerParams(
            collective_id=0, has_side_effects=True, vmem_limit_bytes=60 * 1024 * 1024
        ),
    )(
        start_guess,
        right_side,
        root_diagonal[None, :],
        preconditioner,
        border_block,
        coupling_inverse,
        border_count,
        column_tiles,
    )


def solution(mesh):
    rows = ("scen", "rootr")
    placed = (
        P(rows, "rootc"),
        P(rows, "rootc"),
        P(rows),
        P(rows, None),
        P(rows, "rootc", None),
        P(rows, "rootc", None),
        P(rows),
        P(rows, None),
    )
    return jax.shard_map(
        functools.partial(local, mesh.shape["scen"]),
        mesh=mesh,
        in_specs=placed,
        out_specs=P(rows, "rootc"),
        check_vma=False,
    )
```

```python
import functools
import itertools
import math

import jax
import jax.numpy as jnp
from jax import lax
from jax.experimental import pallas as pl
from jax.experimental.pallas import tpu as pltpu
from jax.sharding import PartitionSpec as P

TILE = 128
MESH = pl.DeviceIdType.MESH
LOW_STEP = 1
OWN_STEP = 2
TERM_STEP = 2
AHEAD = 2


class Place:
    def __init__(self, count):
        self.count, self.hops = count, count // 2
        self.scen, self.core = lax.axis_index("scen"), lax.axis_index("rootr")
        side, level = lax.rem(self.scen, 2), lax.div(self.scen, 2)
        self.spot = level * (1 - side) + (count - 1 - level) * side
        self.ahead = [self.at(1), self.at(count - 1)]

    def at(self, shift):
        spot = lax.rem(self.spot + shift, self.count)
        upper = lax.div(spot, self.hops)
        return (1 - upper) * 2 * spot + upper * (2 * (self.count - 1 - spot) + 1)

    def origin(self, way, hop):
        return self.at(self.count - hop if way == 0 else hop)

    def origins(self, hop):
        if hop == 0:
            return [self.scen]
        if hop == self.hops:
            return [self.origin(0, hop)]
        return [self.origin(0, hop), self.origin(1, hop)]


class Stream:
    def __init__(self, place, hub, buf, rows, step, sems):
        self.hub = hub
        self.place, self.buf, self.rows, self.step = place, buf, rows, step
        self.chunks = rows // step
        self.ring_send, self.ring_recv, self.pair_send, self.pair_recv = sems
        self.forwarded = self.shared = 0

    def piece(self, scen, core, chunk):
        first = (scen * 2 + core) * self.rows + chunk * self.step
        return self.buf.at[pl.ds(first, self.step)]

    def carried(self, way, hop, core):
        return hop < self.place.hops or way == core

    def rounds(self, hop):
        return [
            [
                (way, core, chunk)
                for core in (self.hub, 1 - self.hub)
                for way in range(2)
                if self.carried(way, hop, core)
            ]
            for chunk in range(self.chunks)
        ]

    def ring_copy(self, way, hop, core, chunk, ref):
        slot = ((way * self.place.hops + hop - 1) * 2 + core) * self.chunks + chunk
        return pltpu.make_async_remote_copy(
            src_ref=ref,
            dst_ref=ref,
            send_sem=self.ring_send.at[0],
            recv_sem=self.ring_recv.at[slot],
            device_id={"scen": self.place.ahead[way], "rootr": self.hub},
            device_id_type=MESH,
        )

    def pair_copy(self, hop, ref):
        return pltpu.make_async_remote_copy(
            src_ref=ref,
            dst_ref=ref,
            send_sem=self.pair_send.at[0],
            recv_sem=self.pair_recv.at[hop],
            device_id={"rootr": 1 - self.place.core},
            device_id_type=MESH,
        )

    def send(self, chunks):
        for core in range(2):

            @pl.when(self.place.core == core)
            def start():
                for chunk in chunks:
                    ref = self.piece(self.place.scen, core, chunk)
                    for way in range(2):
                        if self.carried(way, 1, core):
                            self.ring_copy(way, 1, core, chunk, ref).start()

    def share(self):
        own = self.buf.at[pl.ds((self.place.scen * 2 + self.place.core) * self.rows, self.rows)]
        self.pair_copy(0, own).start()

    def begin(self):
        self.send(range(self.chunks))
        self.share()

    def relay(self, hop, arrivals):
        for way, core, chunk in arrivals:
            self.forwarded += self.step * (hop < self.place.hops and self.carried(way, hop + 1, core))
            self.shared += self.step

        @pl.when(self.place.core == self.hub)
        def forward():
            for way, core, chunk in arrivals:
                ref = self.piece(self.place.origin(way, hop), core, chunk)
                self.ring_copy(way, hop, core, chunk, ref).wait_recv()
                if hop < self.place.hops and self.carried(way, hop + 1, core):
                    self.ring_copy(way, hop + 1, core, chunk, ref).start()
                self.pair_copy(self.pair_slot(hop, chunk), ref).start()

    def pair_slot(self, hop, chunk):
        return hop + chunk * (hop == self.place.hops)

    def settle(self, hop, chunks=None):
        if hop == 0:
            self.pair_copy(0, self.buf.at[pl.ds(0, self.rows)]).wait_recv()
            return

        @pl.when(self.place.core != self.hub)
        def arrived():
            if hop < self.place.hops:
                self.pair_copy(hop, self.buf.at[pl.ds(0, 4 * self.rows)]).wait_recv()
                return
            for chunk in range(self.chunks) if chunks is None else chunks:
                ref = self.buf.at[pl.ds(0, 2 * self.step)]
                self.pair_copy(self.pair_slot(hop, chunk), ref).wait_recv()

    def finish(self):
        for core in range(2):
            ways = sum(self.carried(way, 1, core) for way in range(2))
            ring_rows = ways * self.rows + (core == self.hub) * self.forwarded
            pair_rows = self.rows + (core == self.hub) * self.shared

            @pl.when(self.place.core == core)
            def sent():
                ref = self.buf.at[pl.ds(0, ring_rows)]
                self.ring_copy(0, 1, 0, 0, ref).wait_send()
                self.pair_copy(0, self.buf.at[pl.ds(0, pair_rows)]).wait_send()


def kernel(
    count,
    guess_hbm,
    right_hbm,
    diagonal_hbm,
    precon_hbm,
    border_hbm,
    inverse_hbm,
    live_hbm,
    own_tiles_hbm,
    out_ref,
    live_ref,
    own_tiles_ref,
    guess,
    right,
    diagonal,
    low_all,
    own_all,
    term_all,
    tiles_all,
    tiles_smem,
    precon,
    border,
    inverse,
    local_sems,
    cross_send,
    cross_recv,
    *ring_sems,
):
    place = Place(count)
    hops = place.hops
    side = lax.axis_index("rootc")
    own_rows, half_rhs = guess.shape
    half_rows, coupled = border_hbm.shape[1:]
    touched = coupled // TILE
    own_block = place.scen * 2 + place.core

    barrier = pltpu.get_barrier_semaphore()
    peers = [{"scen": scen, "rootr": core} for scen in place.ahead for core in range(2)]
    peers += [{"rootr": 1 - place.core}, {"rootc": 1 - side}]
    for peer in peers:
        pl.semaphore_signal(barrier, inc=1, device_id=peer, device_id_type=MESH)

    load_guess = pltpu.make_async_copy(guess_hbm, guess, local_sems.at[0])
    load_right = pltpu.make_async_copy(right_hbm, right, local_sems.at[1])
    load_diagonal = pltpu.make_async_copy(diagonal_hbm, diagonal, local_sems.at[2])
    own_half = pl.ds(pl.multiple_of(side * half_rows, half_rows), half_rows)
    load_border = pltpu.make_async_copy(border_hbm.at[0], border.at[own_half], local_sems.at[3])
    load_inverse = pltpu.make_async_copy(inverse_hbm.at[0], inverse.at[own_half], local_sems.at[4])
    load_live = pltpu.make_async_copy(live_hbm, live_ref, local_sems.at[7])
    load_tiles = pltpu.make_async_copy(own_tiles_hbm, own_tiles_ref, local_sems.at[8])
    columns_count = precon.shape[0]
    loads = (load_guess, load_tiles, load_right, load_diagonal, load_border, load_inverse, load_live)
    for load in loads:
        load.start()

    unit = low_all.shape[1]
    units = own_rows // unit
    per_tile = TILE // unit
    own_slice = pl.ds(own_block * units, units)
    split = (units, unit, half_rhs)
    load_guess.wait()
    low_all[own_slice] = guess[...].astype(jnp.bfloat16).reshape(split)

    low = Stream(place, 1, low_all, units, min(LOW_STEP, units), ring_sems[0:4])
    own = Stream(place, 0, own_all, units, min(OWN_STEP, units), ring_sems[4:8])
    term = Stream(place, 1, term_all, touched, TERM_STEP, ring_sems[8:12])
    tiles = Stream(place, 1, tiles_all, 1, 1, ring_sems[12:16])

    pl.semaphore_wait(barrier, len(peers))
    low.begin()
    crossings = []
    for index, (source, target) in enumerate(((border_hbm, border), (inverse_hbm, inverse))):
        crossing = pltpu.make_async_remote_copy(
            src_ref=source.at[0],
            dst_ref=target.at[own_half],
            send_sem=cross_send.at[index],
            recv_sem=cross_recv.at[index],
            device_id={"rootc": 1 - side},
            device_id_type=MESH,
        )
        crossing.start()
        crossings.append(crossing)
    load_tiles.wait()
    lanes = lax.broadcasted_iota(jnp.int32, (1, 1, TILE), 2)
    tiles_row = jnp.zeros((1, 1, TILE), jnp.int32)
    for k in range(touched):
        tiles_row = jnp.where(lanes == k, own_tiles_ref[0, k], tiles_row)
    tiles_all[pl.ds(own_block, 1)] = tiles_row
    tiles.begin()

    load_right.wait()
    load_diagonal.wait()
    scale = jnp.broadcast_to(diagonal[...], (half_rhs, own_rows)).T
    own_terms = right[...] - scale * guess[...]
    own_all[own_slice] = own_terms.astype(jnp.bfloat16).reshape(split)

    @pl.loop(0, columns_count)
    def start_column(t):
        columns = pl.ds(pl.multiple_of(t * TILE, TILE), TILE)
        pltpu.make_async_copy(precon_hbm.at[:, columns], precon.at[t], local_sems.at[5]).start()

    for hop in range(1, hops + 1):
        for arrivals in low.rounds(hop):
            low.relay(hop, arrivals)
        if hop == max(hops - AHEAD, 1):
            low.settle(hop)
            own.begin()
        for arrivals in tiles.rounds(hop):
            tiles.relay(hop, arrivals)
    flow = [(hop, arrivals) for hop in range(1, hops + 1) for arrivals in own.rounds(hop)]

    def drain(stop):
        while flow and flow[0][0] <= stop:
            own.relay(*flow.pop(0))

    drain(1)
    for hop in range(hops + 1):
        if hop == hops:
            own.relay(*flow.pop(0))
        if hop != max(hops - AHEAD, 1):
            low.settle(hop)

    def product(columns, values, rows):
        left = jnp.concatenate([precon[t] for t in columns], axis=1)
        right = jnp.concatenate([values[t] for t in rows], axis=0)
        return jnp.dot(left, right, preferred_element_type=jnp.float32)

    own_tiles = own_rows // TILE

    def add_own(block):
        total = jnp.zeros_like(out_ref)
        for k in range(0, own_tiles, 2):
            group = [block * own_tiles + j for j in range(k, min(k + 2, own_tiles))]
            total = total + product(group, own_all, group)
        out_ref[...] += total

    def add_term(*blocks, tiles=range(touched)):
        total = jnp.zeros_like(out_ref)
        for block, k in itertools.product(blocks, tiles[::2]):
            group = range(k, min(k + 2, tiles[-1] + 1))
            total = total + product(
                [tiles_smem[block, 0, j] for j in group],
                term_all,
                [block * touched + j for j in group],
            )
        out_ref[...] += total

    def work(stream, add, hop):
        blocks = [scen * 2 + core for core in range(2) for scen in place.origins(hop)]
        return [lambda: stream.settle(hop)] + [functools.partial(add, block) for block in blocks]

    def add_last(chunk):
        term.settle(hops, [chunk])
        last = place.origin(0, hops) * 2
        tiles = range(chunk * term.step, (chunk + 1) * term.step)
        add_term(last, last + 1, tiles=tiles)

    def run(todo, count):
        for _ in range(min(count, len(todo))):
            todo.pop(0)()

    whole_tiles = own_rows % TILE == 0
    load_border.wait()
    crossings[0].wait_recv()
    load_live.wait()
    live = jnp.clip(live_ref[0], 0, 2 * half_rows)
    live_mask = lax.broadcasted_iota(jnp.int32, (2 * half_rows, half_rhs), 0) < live
    picked = jnp.concatenate(
        [
            low_all[own_tiles_ref[0, k] * per_tile + part]
            for k in range(touched)
            for part in range(per_tile)
        ],
        axis=0,
    )
    values = jnp.dot(border[...], picked, preferred_element_type=jnp.float32)
    values = jnp.where(live_mask, values, 0.0).astype(jnp.bfloat16)
    drain(2)
    pltpu.make_async_copy(precon, precon, local_sems.at[5]).wait()
    out_ref[...] = guess[...]
    todo = work(own, add_own, 0) + work(own, add_own, 1) if whole_tiles else []
    run(todo, len(todo))
    load_inverse.wait()
    crossings[1].wait_recv()
    solved = jnp.dot(inverse[...], values, preferred_element_type=jnp.float32)
    solved = jnp.where(live_mask, solved, 0.0).astype(jnp.bfloat16)
    width = term.step * TILE
    for chunk in range(term.chunks):
        left = border[:, pl.ds(chunk * width, width)]
        terms = lax.dot_general(
            left, solved, (((0,), (0,)), ((), ())), preferred_element_type=jnp.float32
        )
        term_all[pl.ds(own_block * touched + chunk * term.step, term.step)] = terms.astype(
            jnp.bfloat16
        ).reshape(term.step, TILE, half_rhs)
        if chunk:
            term.send([chunk - 1])
    term.send([term.chunks - 1])
    term.share()

    for hop in range(hops + 1):
        tiles.settle(hop)
    to_smem = pltpu.make_async_copy(tiles_all, tiles_smem, local_sems.at[6])
    to_smem.start()
    to_smem.wait()

    todo = []
    for hop in range(1, hops + 1):
        todo += work(term, add_term, hop - 1)
        if whole_tiles and hop > 1:
            todo += work(own, add_own, hop)
        rounds = term.rounds(hop)
        share = -(-len(todo) // len(rounds))
        for arrivals in rounds:
            if flow:
                own.relay(*flow.pop(0))
            term.relay(hop, arrivals)
            if flow and flow[0][0] <= hop:
                own.relay(*flow.pop(0))
            run(todo, share)
            if hop == hops and arrivals[0][2]:
                add_last(arrivals[0][2] - 1)
        drain(hop + 1)
        run(todo, len(todo))
    add_last(term.chunks - 1)
    if not whole_tiles:
        for hop in range(hops + 1):
            own.settle(hop)

        @pl.loop(0, columns_count)
        def add_column(t):
            rows = [t * per_tile + part for part in range(per_tile)]
            out_ref[...] += product([t], own_all, rows)

    drain(hops)
    for stream in (low, own, term, tiles):
        stream.finish()
    for crossing in crossings:
        crossing.wait_send()


def local(
    count,
    start_guess,
    right_side,
    root_diagonal,
    preconditioner,
    border_block,
    coupling_inverse,
    border_count,
    column_tiles,
):
    own_rows, half_rhs = start_guess.shape
    order = preconditioner.shape[1]
    half_rows, coupled = border_block.shape[1:]
    blocks = count * 2
    touched = column_tiles.shape[1]
    hops = count // 2
    ring_sems = []
    unit = math.gcd(own_rows, TILE)
    units = own_rows // unit
    for rows, step in ((units, LOW_STEP), (units, OWN_STEP), (touched, TERM_STEP), (1, 1)):
        chunks = rows // min(step, rows)
        ring_sems += [
            pltpu.SemaphoreType.DMA((1,)),
            pltpu.SemaphoreType.DMA((4 * hops * chunks,)),
            pltpu.SemaphoreType.DMA((1,)),
            pltpu.SemaphoreType.DMA((hops + chunks,)),
        ]
    vmem = pl.BlockSpec(memory_space=pltpu.VMEM)
    anywhere = pl.BlockSpec(memory_space=pltpu.HBM)
    return pl.pallas_call(
        functools.partial(kernel, count),
        out_shape=pltpu.VMEM((own_rows, half_rhs), jnp.float32),
        in_specs=[anywhere] * 8,
        out_specs=vmem,
        scratch_shapes=[
            pltpu.SMEM(border_count.shape, jnp.int32),
            pltpu.SMEM(column_tiles.shape, jnp.int32),
            pltpu.VMEM((own_rows, half_rhs), jnp.float32),
            pltpu.VMEM((own_rows, half_rhs), jnp.float32),
            pltpu.VMEM((1, own_rows), jnp.float32),
            pltpu.VMEM((order // unit, unit, half_rhs), jnp.bfloat16),
            pltpu.VMEM((order // unit, unit, half_rhs), jnp.bfloat16),
            pltpu.VMEM((blocks * touched, TILE, half_rhs), jnp.bfloat16),
            pltpu.VMEM((blocks, 1, TILE), jnp.int32),
            pltpu.SMEM((blocks, 1, TILE), jnp.int32),
            pltpu.VMEM((order // TILE, own_rows, TILE), jnp.bfloat16),
            pltpu.VMEM((2 * half_rows, coupled), jnp.bfloat16),
            pltpu.VMEM((2 * half_rows, 2 * half_rows), jnp.bfloat16),
            pltpu.SemaphoreType.DMA((9,)),
            pltpu.SemaphoreType.DMA((2,)),
            pltpu.SemaphoreType.DMA((2,)),
        ]
        + ring_sems,
        compiler_params=pltpu.CompilerParams(
            collective_id=0, has_side_effects=True, vmem_limit_bytes=60 * 1024 * 1024
        ),
    )(
        start_guess,
        right_side,
        root_diagonal[None, :],
        preconditioner,
        border_block,
        coupling_inverse,
        border_count,
        column_tiles,
    )


def solution(mesh):
    rows = ("scen", "rootr")
    placed = (
        P(rows, "rootc"),
        P(rows, "rootc"),
        P(rows),
        P(rows, None),
        P(rows, "rootc", None),
        P(rows, "rootc", None),
        P(rows),
        P(rows, None),
    )
    return jax.shard_map(
        functools.partial(local, mesh.shape["scen"]),
        mesh=mesh,
        in_specs=placed,
        out_specs=P(rows, "rootc"),
        check_vma=False,
    )
```

```python
import functools
import itertools
import math

import jax
import jax.numpy as jnp
from jax import lax
from jax.experimental import pallas as pl
from jax.experimental.pallas import tpu as pltpu
from jax.sharding import PartitionSpec as P

TILE = 128
MESH = pl.DeviceIdType.MESH
LOW_STEP = 1
OWN_STEP = 2
TERM_STEP = 2
AHEAD = 2


class Place:
    def __init__(self, count):
        self.count, self.hops = count, count // 2
        self.scen, self.core = lax.axis_index("scen"), lax.axis_index("rootr")
        side, level = lax.rem(self.scen, 2), lax.div(self.scen, 2)
        self.spot = level * (1 - side) + (count - 1 - level) * side
        self.ahead = [self.at(1), self.at(count - 1)]

    def at(self, shift):
        spot = lax.rem(self.spot + shift, self.count)
        upper = lax.div(spot, self.hops)
        return (1 - upper) * 2 * spot + upper * (2 * (self.count - 1 - spot) + 1)

    def origin(self, way, hop):
        return self.at(self.count - hop if way == 0 else hop)

    def origins(self, hop):
        if hop == 0:
            return [self.scen]
        if hop == self.hops:
            return [self.origin(0, hop)]
        return [self.origin(0, hop), self.origin(1, hop)]


class Stream:
    def __init__(self, place, hub, buf, rows, step, sems):
        self.hub = hub
        self.place, self.buf, self.rows, self.step = place, buf, rows, step
        self.chunks = rows // step
        self.ring_send, self.ring_recv, self.pair_send, self.pair_recv = sems
        self.forwarded = self.shared = 0

    def piece(self, scen, core, chunk):
        first = (scen * 2 + core) * self.rows + chunk * self.step
        return self.buf.at[pl.ds(first, self.step)]

    def carried(self, way, hop, core):
        return hop < self.place.hops or way == core

    def rounds(self, hop):
        return [
            [
                (way, core, chunk)
                for core in (self.hub, 1 - self.hub)
                for way in range(2)
                if self.carried(way, hop, core)
            ]
            for chunk in range(self.chunks)
        ]

    def ring_copy(self, way, hop, core, chunk, ref):
        slot = ((way * self.place.hops + hop - 1) * 2 + core) * self.chunks + chunk
        return pltpu.make_async_remote_copy(
            src_ref=ref,
            dst_ref=ref,
            send_sem=self.ring_send.at[0],
            recv_sem=self.ring_recv.at[slot],
            device_id={"scen": self.place.ahead[way], "rootr": self.hub},
            device_id_type=MESH,
        )

    def pair_copy(self, hop, ref):
        return pltpu.make_async_remote_copy(
            src_ref=ref,
            dst_ref=ref,
            send_sem=self.pair_send.at[0],
            recv_sem=self.pair_recv.at[hop],
            device_id={"rootr": 1 - self.place.core},
            device_id_type=MESH,
        )

    def send(self, chunks):
        for core in range(2):

            @pl.when(self.place.core == core)
            def start():
                for chunk in chunks:
                    ref = self.piece(self.place.scen, core, chunk)
                    for way in range(2):
                        if self.carried(way, 1, core):
                            self.ring_copy(way, 1, core, chunk, ref).start()

    def share(self):
        own = self.buf.at[pl.ds((self.place.scen * 2 + self.place.core) * self.rows, self.rows)]
        self.pair_copy(0, own).start()

    def begin(self):
        self.send(range(self.chunks))
        self.share()

    def relay(self, hop, arrivals):
        for way, core, chunk in arrivals:
            self.forwarded += self.step * (hop < self.place.hops and self.carried(way, hop + 1, core))
            self.shared += self.step

        @pl.when(self.place.core == self.hub)
        def forward():
            for way, core, chunk in arrivals:
                ref = self.piece(self.place.origin(way, hop), core, chunk)
                self.ring_copy(way, hop, core, chunk, ref).wait_recv()
                if hop < self.place.hops and self.carried(way, hop + 1, core):
                    self.ring_copy(way, hop + 1, core, chunk, ref).start()
                self.pair_copy(self.pair_slot(hop, chunk), ref).start()

    def pair_slot(self, hop, chunk):
        return hop + chunk * (hop == self.place.hops)

    def settle(self, hop, chunks=None):
        if hop == 0:
            self.pair_copy(0, self.buf.at[pl.ds(0, self.rows)]).wait_recv()
            return

        @pl.when(self.place.core != self.hub)
        def arrived():
            if hop < self.place.hops:
                self.pair_copy(hop, self.buf.at[pl.ds(0, 4 * self.rows)]).wait_recv()
                return
            for chunk in range(self.chunks) if chunks is None else chunks:
                ref = self.buf.at[pl.ds(0, 2 * self.step)]
                self.pair_copy(self.pair_slot(hop, chunk), ref).wait_recv()

    def finish(self):
        for core in range(2):
            ways = sum(self.carried(way, 1, core) for way in range(2))
            ring_rows = ways * self.rows + (core == self.hub) * self.forwarded
            pair_rows = self.rows + (core == self.hub) * self.shared

            @pl.when(self.place.core == core)
            def sent():
                ref = self.buf.at[pl.ds(0, ring_rows)]
                self.ring_copy(0, 1, 0, 0, ref).wait_send()
                self.pair_copy(0, self.buf.at[pl.ds(0, pair_rows)]).wait_send()


def kernel(
    count,
    guess_hbm,
    right_hbm,
    diagonal_hbm,
    precon_hbm,
    border_hbm,
    inverse_hbm,
    live_hbm,
    own_tiles_hbm,
    out_ref,
    live_ref,
    own_tiles_ref,
    guess,
    right,
    diagonal,
    low_all,
    own_all,
    term_all,
    tiles_all,
    tiles_smem,
    precon,
    border,
    inverse,
    local_sems,
    cross_send,
    cross_recv,
    *ring_sems,
):
    place = Place(count)
    hops = place.hops
    side = lax.axis_index("rootc")
    own_rows, half_rhs = guess.shape
    half_rows, coupled = border_hbm.shape[1:]
    touched = coupled // TILE
    own_block = place.scen * 2 + place.core

    barrier = pltpu.get_barrier_semaphore()
    peers = [{"scen": scen, "rootr": core} for scen in place.ahead for core in range(2)]
    peers += [{"rootr": 1 - place.core}, {"rootc": 1 - side}]
    for peer in peers:
        pl.semaphore_signal(barrier, inc=1, device_id=peer, device_id_type=MESH)

    load_guess = pltpu.make_async_copy(guess_hbm, guess, local_sems.at[0])
    load_right = pltpu.make_async_copy(right_hbm, right, local_sems.at[1])
    load_diagonal = pltpu.make_async_copy(diagonal_hbm, diagonal, local_sems.at[2])
    own_half = pl.ds(pl.multiple_of(side * half_rows, half_rows), half_rows)
    load_border = pltpu.make_async_copy(border_hbm.at[0], border.at[own_half], local_sems.at[3])
    load_inverse = pltpu.make_async_copy(inverse_hbm.at[0], inverse.at[own_half], local_sems.at[4])
    load_live = pltpu.make_async_copy(live_hbm, live_ref, local_sems.at[7])
    load_tiles = pltpu.make_async_copy(own_tiles_hbm, own_tiles_ref, local_sems.at[8])
    columns_count = precon.shape[0]
    loads = (load_guess, load_tiles, load_right, load_diagonal, load_border, load_inverse, load_live)
    for load in loads:
        load.start()

    unit = low_all.shape[1]
    units = own_rows // unit
    per_tile = TILE // unit
    own_slice = pl.ds(own_block * units, units)
    split = (units, unit, half_rhs)
    load_guess.wait()
    low_all[own_slice] = guess[...].astype(jnp.bfloat16).reshape(split)

    low = Stream(place, 1, low_all, units, min(LOW_STEP, units), ring_sems[0:4])
    own = Stream(place, 0, own_all, units, min(OWN_STEP, units), ring_sems[4:8])
    term = Stream(place, 1, term_all, touched, TERM_STEP, ring_sems[8:12])
    tiles = Stream(place, 1, tiles_all, 1, 1, ring_sems[12:16])

    pl.semaphore_wait(barrier, len(peers))
    low.begin()
    crossings = []
    for index, (source, target) in enumerate(((border_hbm, border), (inverse_hbm, inverse))):
        crossing = pltpu.make_async_remote_copy(
            src_ref=source.at[0],
            dst_ref=target.at[own_half],
            send_sem=cross_send.at[index],
            recv_sem=cross_recv.at[index],
            device_id={"rootc": 1 - side},
            device_id_type=MESH,
        )
        crossing.start()
        crossings.append(crossing)
    load_tiles.wait()
    lanes = lax.broadcasted_iota(jnp.int32, (1, 1, TILE), 2)
    tiles_row = jnp.zeros((1, 1, TILE), jnp.int32)
    for k in range(touched):
        tiles_row = jnp.where(lanes == k, own_tiles_ref[0, k], tiles_row)
    tiles_all[pl.ds(own_block, 1)] = tiles_row
    tiles.begin()

    load_right.wait()
    load_diagonal.wait()
    scale = jnp.broadcast_to(diagonal[...], (half_rhs, own_rows)).T
    own_terms = right[...] - scale * guess[...]
    own_all[own_slice] = own_terms.astype(jnp.bfloat16).reshape(split)

    @pl.loop(0, columns_count)
    def start_column(t):
        columns = pl.ds(pl.multiple_of(t * TILE, TILE), TILE)
        pltpu.make_async_copy(precon_hbm.at[:, columns], precon.at[t], local_sems.at[5]).start()

    for hop in range(1, hops + 1):
        for arrivals in low.rounds(hop):
            low.relay(hop, arrivals)
        if hop == max(hops - AHEAD, 1):
            low.settle(hop)
            own.begin()
        for arrivals in tiles.rounds(hop):
            tiles.relay(hop, arrivals)
    flow = [(hop, arrivals) for hop in range(1, hops + 1) for arrivals in own.rounds(hop)]

    def drain(stop):
        while flow and flow[0][0] <= stop:
            own.relay(*flow.pop(0))

    drain(1)
    for hop in range(hops + 1):
        if hop == hops:
            own.relay(*flow.pop(0))
        if hop != max(hops - AHEAD, 1):
            low.settle(hop)

    def product(columns, values, rows):
        left = jnp.concatenate([precon[t] for t in columns], axis=1)
        right = jnp.concatenate([values[t] for t in rows], axis=0)
        return jnp.dot(left, right, preferred_element_type=jnp.float32)

    own_tiles = own_rows // TILE

    def add_own(block):
        total = jnp.zeros_like(out_ref)
        for k in range(0, own_tiles, 2):
            group = [block * own_tiles + j for j in range(k, min(k + 2, own_tiles))]
            total = total + product(group, own_all, group)
        out_ref[...] += total

    def add_term(*blocks, tiles=range(touched)):
        total = jnp.zeros_like(out_ref)
        for block, k in itertools.product(blocks, tiles[::2]):
            group = range(k, min(k + 2, tiles[-1] + 1))
            total = total + product(
                [tiles_smem[block, 0, j] for j in group],
                term_all,
                [block * touched + j for j in group],
            )
        out_ref[...] += total

    def work(stream, add, hop):
        blocks = [scen * 2 + core for core in range(2) for scen in place.origins(hop)]
        return [lambda: stream.settle(hop)] + [functools.partial(add, block) for block in blocks]

    def add_last(chunk):
        term.settle(hops, [chunk])
        last = place.origin(0, hops) * 2
        tiles = range(chunk * term.step, (chunk + 1) * term.step)
        add_term(last, last + 1, tiles=tiles)

    def run(todo, count):
        for _ in range(min(count, len(todo))):
            todo.pop(0)()

    whole_tiles = own_rows % TILE == 0
    load_border.wait()
    crossings[0].wait_recv()
    load_live.wait()
    live = jnp.clip(live_ref[0, 0], 0, 2 * half_rows)
    live_mask = lax.broadcasted_iota(jnp.int32, (2 * half_rows, half_rhs), 0) < live
    picked = jnp.concatenate(
        [
            low_all[own_tiles_ref[0, k] * per_tile + part]
            for k in range(touched)
            for part in range(per_tile)
        ],
        axis=0,
    )
    values = jnp.dot(border[...], picked, preferred_element_type=jnp.float32)
    values = jnp.where(live_mask, values, 0.0).astype(jnp.bfloat16)
    drain(2)
    pltpu.make_async_copy(precon, precon, local_sems.at[5]).wait()
    out_ref[...] = guess[...]
    todo = work(own, add_own, 0) + work(own, add_own, 1) if whole_tiles else []
    run(todo, len(todo))
    load_inverse.wait()
    crossings[1].wait_recv()
    solved = jnp.dot(inverse[...], values, preferred_element_type=jnp.float32)
    solved = jnp.where(live_mask, solved, 0.0).astype(jnp.bfloat16)
    width = term.step * TILE
    for chunk in range(term.chunks):
        left = border[:, pl.ds(chunk * width, width)]
        terms = lax.dot_general(
            left, solved, (((0,), (0,)), ((), ())), preferred_element_type=jnp.float32
        )
        term_all[pl.ds(own_block * touched + chunk * term.step, term.step)] = terms.astype(
            jnp.bfloat16
        ).reshape(term.step, TILE, half_rhs)
        if chunk:
            term.send([chunk - 1])
    term.send([term.chunks - 1])
    term.share()

    for hop in range(hops + 1):
        tiles.settle(hop)
    to_smem = pltpu.make_async_copy(tiles_all, tiles_smem, local_sems.at[6])
    to_smem.start()
    to_smem.wait()

    todo = []
    for hop in range(1, hops + 1):
        todo += work(term, add_term, hop - 1)
        if whole_tiles and hop < hops:
            todo = work(own, add_own, hop + 1) + todo
        rounds = term.rounds(hop)
        share = -(-len(todo) // len(rounds))
        for arrivals in rounds:
            if flow:
                own.relay(*flow.pop(0))
            term.relay(hop, arrivals)
            if flow and flow[0][0] <= hop:
                own.relay(*flow.pop(0))
            run(todo, share)
            if hop == hops and arrivals[0][2]:
                add_last(arrivals[0][2] - 1)
        drain(hop + 1)
        run(todo, len(todo))
    add_last(term.chunks - 1)
    if not whole_tiles:
        for hop in range(hops + 1):
            own.settle(hop)

        @pl.loop(0, columns_count)
        def add_column(t):
            rows = [t * per_tile + part for part in range(per_tile)]
            out_ref[...] += product([t], own_all, rows)

    drain(hops)
    for stream in (low, own, term, tiles):
        stream.finish()
    for crossing in crossings:
        crossing.wait_send()


def local(
    count,
    start_guess,
    right_side,
    root_diagonal,
    preconditioner,
    border_block,
    coupling_inverse,
    border_count,
    column_tiles,
):
    own_rows, half_rhs = start_guess.shape
    order = preconditioner.shape[1]
    half_rows, coupled = border_block.shape[1:]
    blocks = count * 2
    touched = column_tiles.shape[1]
    hops = count // 2
    ring_sems = []
    unit = math.gcd(own_rows, TILE)
    units = own_rows // unit
    for rows, step in ((units, LOW_STEP), (units, OWN_STEP), (touched, TERM_STEP), (1, 1)):
        chunks = rows // min(step, rows)
        ring_sems += [
            pltpu.SemaphoreType.DMA((1,)),
            pltpu.SemaphoreType.DMA((4 * hops * chunks,)),
            pltpu.SemaphoreType.DMA((1,)),
            pltpu.SemaphoreType.DMA((hops + chunks,)),
        ]
    vmem = pl.BlockSpec(memory_space=pltpu.VMEM)
    anywhere = pl.BlockSpec(memory_space=pltpu.HBM)
    return pl.pallas_call(
        functools.partial(kernel, count),
        out_shape=pltpu.VMEM((own_rows, half_rhs), jnp.float32),
        in_specs=[anywhere] * 8,
        out_specs=vmem,
        scratch_shapes=[
            pltpu.SMEM((1,) + border_count.shape, jnp.int32),
            pltpu.SMEM(column_tiles.shape, jnp.int32),
            pltpu.VMEM((own_rows, half_rhs), jnp.float32),
            pltpu.VMEM((own_rows, half_rhs), jnp.float32),
            pltpu.VMEM((1, own_rows), jnp.float32),
            pltpu.VMEM((order // unit, unit, half_rhs), jnp.bfloat16),
            pltpu.VMEM((order // unit, unit, half_rhs), jnp.bfloat16),
            pltpu.VMEM((blocks * touched, TILE, half_rhs), jnp.bfloat16),
            pltpu.VMEM((blocks, 1, TILE), jnp.int32),
            pltpu.SMEM((blocks, 1, TILE), jnp.int32),
            pltpu.VMEM((order // TILE, own_rows, TILE), jnp.bfloat16),
            pltpu.VMEM((2 * half_rows, coupled), jnp.bfloat16),
            pltpu.VMEM((2 * half_rows, 2 * half_rows), jnp.bfloat16),
            pltpu.SemaphoreType.DMA((9,)),
            pltpu.SemaphoreType.DMA((2,)),
            pltpu.SemaphoreType.DMA((2,)),
        ]
        + ring_sems,
        compiler_params=pltpu.CompilerParams(
            collective_id=0, has_side_effects=True, vmem_limit_bytes=60 * 1024 * 1024
        ),
    )(
        start_guess,
        right_side,
        root_diagonal[None, :],
        preconditioner,
        border_block,
        coupling_inverse,
        border_count[None, :],
        column_tiles,
    )


def solution(mesh):
    rows = ("scen", "rootr")
    placed = (
        P(rows, "rootc"),
        P(rows, "rootc"),
        P(rows),
        P(rows, None),
        P(rows, "rootc", None),
        P(rows, "rootc", None),
        P(rows),
        P(rows, None),
    )
    return jax.shard_map(
        functools.partial(local, mesh.shape["scen"]),
        mesh=mesh,
        in_specs=placed,
        out_specs=P(rows, "rootc"),
        check_vma=False,
    )
```

```python
import functools
import itertools
import math

import jax
import jax.numpy as jnp
from jax import lax
from jax.experimental import pallas as pl
from jax.experimental.pallas import tpu as pltpu
from jax.sharding import PartitionSpec as P

TILE = 128
MESH = pl.DeviceIdType.MESH
LOW_STEP = 1
OWN_STEP = 2
TERM_STEP = 2
AHEAD = 2


class Place:
    def __init__(self, count):
        self.count, self.hops = count, count // 2
        self.scen, self.core = lax.axis_index("scen"), lax.axis_index("rootr")
        side, level = lax.rem(self.scen, 2), lax.div(self.scen, 2)
        self.spot = level * (1 - side) + (count - 1 - level) * side
        self.ahead = [self.at(1), self.at(count - 1)]

    def at(self, shift):
        spot = lax.rem(self.spot + shift, self.count)
        upper = lax.div(spot, self.hops)
        return (1 - upper) * 2 * spot + upper * (2 * (self.count - 1 - spot) + 1)

    def origin(self, way, hop):
        return self.at(self.count - hop if way == 0 else hop)

    def origins(self, hop):
        if hop == 0:
            return [self.scen]
        if hop == self.hops:
            return [self.origin(0, hop)]
        return [self.origin(0, hop), self.origin(1, hop)]


class Stream:
    def __init__(self, place, hub, buf, rows, step, sems):
        self.hub = hub
        self.place, self.buf, self.rows, self.step = place, buf, rows, step
        self.chunks = rows // step
        self.ring_send, self.ring_recv, self.pair_send, self.pair_recv = sems
        self.forwarded = self.shared = 0

    def piece(self, scen, core, chunk):
        first = (scen * 2 + core) * self.rows + chunk * self.step
        return self.buf.at[pl.ds(first, self.step)]

    def carried(self, way, hop, core):
        return hop < self.place.hops or way == core

    def rounds(self, hop):
        return [
            [
                (way, core, chunk)
                for core in (self.hub, 1 - self.hub)
                for way in range(2)
                if self.carried(way, hop, core)
            ]
            for chunk in range(self.chunks)
        ]

    def ring_copy(self, way, hop, core, chunk, ref):
        slot = ((way * self.place.hops + hop - 1) * 2 + core) * self.chunks + chunk
        return pltpu.make_async_remote_copy(
            src_ref=ref,
            dst_ref=ref,
            send_sem=self.ring_send.at[0],
            recv_sem=self.ring_recv.at[slot],
            device_id={"scen": self.place.ahead[way], "rootr": self.hub},
            device_id_type=MESH,
        )

    def pair_copy(self, hop, ref):
        return pltpu.make_async_remote_copy(
            src_ref=ref,
            dst_ref=ref,
            send_sem=self.pair_send.at[0],
            recv_sem=self.pair_recv.at[hop],
            device_id={"rootr": 1 - self.place.core},
            device_id_type=MESH,
        )

    def send(self, chunks):
        for core in range(2):

            @pl.when(self.place.core == core)
            def start():
                for chunk in chunks:
                    ref = self.piece(self.place.scen, core, chunk)
                    for way in range(2):
                        if self.carried(way, 1, core):
                            self.ring_copy(way, 1, core, chunk, ref).start()

    def share(self):
        own = self.buf.at[pl.ds((self.place.scen * 2 + self.place.core) * self.rows, self.rows)]
        self.pair_copy(0, own).start()

    def begin(self):
        self.send(range(self.chunks))
        self.share()

    def relay(self, hop, arrivals):
        for way, core, chunk in arrivals:
            self.forwarded += self.step * (hop < self.place.hops and self.carried(way, hop + 1, core))
            self.shared += self.step

        @pl.when(self.place.core == self.hub)
        def forward():
            for way, core, chunk in arrivals:
                ref = self.piece(self.place.origin(way, hop), core, chunk)
                self.ring_copy(way, hop, core, chunk, ref).wait_recv()
                if hop < self.place.hops and self.carried(way, hop + 1, core):
                    self.ring_copy(way, hop + 1, core, chunk, ref).start()
                self.pair_copy(self.pair_slot(hop, chunk), ref).start()

    def pair_slot(self, hop, chunk):
        return hop + chunk * (hop == self.place.hops)

    def settle(self, hop, chunks=None):
        if hop == 0:
            self.pair_copy(0, self.buf.at[pl.ds(0, self.rows)]).wait_recv()
            return

        @pl.when(self.place.core != self.hub)
        def arrived():
            if hop < self.place.hops:
                self.pair_copy(hop, self.buf.at[pl.ds(0, 4 * self.rows)]).wait_recv()
                return
            for chunk in range(self.chunks) if chunks is None else chunks:
                ref = self.buf.at[pl.ds(0, 2 * self.step)]
                self.pair_copy(self.pair_slot(hop, chunk), ref).wait_recv()

    def finish(self):
        for core in range(2):
            ways = sum(self.carried(way, 1, core) for way in range(2))
            ring_rows = ways * self.rows + (core == self.hub) * self.forwarded
            pair_rows = self.rows + (core == self.hub) * self.shared

            @pl.when(self.place.core == core)
            def sent():
                ref = self.buf.at[pl.ds(0, ring_rows)]
                self.ring_copy(0, 1, 0, 0, ref).wait_send()
                self.pair_copy(0, self.buf.at[pl.ds(0, pair_rows)]).wait_send()


def kernel(
    count,
    guess_hbm,
    right_hbm,
    diagonal_hbm,
    precon_hbm,
    border_hbm,
    inverse_hbm,
    live_hbm,
    own_tiles_hbm,
    out_ref,
    live_ref,
    own_tiles_ref,
    guess,
    right,
    diagonal,
    low_all,
    own_all,
    term_all,
    tiles_all,
    tiles_smem,
    precon,
    border,
    inverse,
    near_terms,
    local_sems,
    cross_send,
    cross_recv,
    *ring_sems,
):
    place = Place(count)
    hops = place.hops
    side = lax.axis_index("rootc")
    own_rows, half_rhs = guess.shape
    half_rows, coupled = border_hbm.shape[1:]
    touched = coupled // TILE
    own_block = place.scen * 2 + place.core

    barrier = pltpu.get_barrier_semaphore()
    peers = [{"scen": scen, "rootr": core} for scen in place.ahead for core in range(2)]
    peers += [{"rootr": 1 - place.core}, {"rootc": 1 - side}]
    for peer in peers:
        pl.semaphore_signal(barrier, inc=1, device_id=peer, device_id_type=MESH)

    load_guess = pltpu.make_async_copy(guess_hbm, guess, local_sems.at[0])
    load_right = pltpu.make_async_copy(right_hbm, right, local_sems.at[1])
    load_diagonal = pltpu.make_async_copy(diagonal_hbm, diagonal, local_sems.at[2])
    own_half = pl.ds(pl.multiple_of(side * half_rows, half_rows), half_rows)
    load_border = pltpu.make_async_copy(border_hbm.at[0], border.at[own_half], local_sems.at[3])
    load_inverse = pltpu.make_async_copy(inverse_hbm.at[0], inverse.at[own_half], local_sems.at[4])
    load_live = pltpu.make_async_copy(live_hbm, live_ref, local_sems.at[7])
    load_tiles = pltpu.make_async_copy(own_tiles_hbm, own_tiles_ref, local_sems.at[8])
    columns_count = precon.shape[0]
    loads = (load_guess, load_tiles, load_right, load_diagonal, load_border, load_inverse, load_live)
    for load in loads:
        load.start()

    unit = low_all.shape[1]
    units = own_rows // unit
    per_tile = TILE // unit
    own_slice = pl.ds(own_block * units, units)
    split = (units, unit, half_rhs)
    load_guess.wait()
    low_all[own_slice] = guess[...].astype(jnp.bfloat16).reshape(split)

    low = Stream(place, 1, low_all, units, min(LOW_STEP, units), ring_sems[0:4])
    own = Stream(place, 0, own_all, units, min(OWN_STEP, units), ring_sems[4:8])
    term = Stream(place, 1, term_all, touched, TERM_STEP, ring_sems[8:12])
    tiles = Stream(place, 1, tiles_all, 1, 1, ring_sems[12:16])

    pl.semaphore_wait(barrier, len(peers))
    low.begin()
    crossings = []
    for index, (source, target) in enumerate(((border_hbm, border), (inverse_hbm, inverse))):
        crossing = pltpu.make_async_remote_copy(
            src_ref=source.at[0],
            dst_ref=target.at[own_half],
            send_sem=cross_send.at[index],
            recv_sem=cross_recv.at[index],
            device_id={"rootc": 1 - side},
            device_id_type=MESH,
        )
        crossing.start()
        crossings.append(crossing)
    load_tiles.wait()
    lanes = lax.broadcasted_iota(jnp.int32, (1, 1, TILE), 2)
    tiles_row = jnp.zeros((1, 1, TILE), jnp.int32)
    for k in range(touched):
        tiles_row = jnp.where(lanes == k, own_tiles_ref[0, k], tiles_row)
    tiles_all[pl.ds(own_block, 1)] = tiles_row
    tiles.begin()

    load_right.wait()
    load_diagonal.wait()
    scale = jnp.broadcast_to(diagonal[...], (half_rhs, own_rows)).T
    own_terms = right[...] - scale * guess[...]
    own_all[own_slice] = own_terms.astype(jnp.bfloat16).reshape(split)

    @pl.loop(0, columns_count)
    def start_column(t):
        columns = pl.ds(pl.multiple_of(t * TILE, TILE), TILE)
        pltpu.make_async_copy(precon_hbm.at[:, columns], precon.at[t], local_sems.at[5]).start()

    for hop in range(1, hops + 1):
        for arrivals in low.rounds(hop):
            low.relay(hop, arrivals)
        if hop == max(hops - AHEAD, 1):
            low.settle(hop)
            own.begin()
        for arrivals in tiles.rounds(hop):
            tiles.relay(hop, arrivals)
    flow = [(hop, arrivals) for hop in range(1, hops + 1) for arrivals in own.rounds(hop)]

    def drain(stop):
        while flow and flow[0][0] <= stop:
            own.relay(*flow.pop(0))

    drain(1)
    for hop in range(hops + 1):
        if hop == hops:
            own.relay(*flow.pop(0))
        if hop != max(hops - AHEAD, 1):
            low.settle(hop)

    def product(columns, values, rows):
        left = jnp.concatenate([precon[t] for t in columns], axis=1)
        right = jnp.concatenate([values[t] for t in rows], axis=0)
        return jnp.dot(left, right, preferred_element_type=jnp.float32)

    own_tiles = own_rows // TILE

    def add_own(block):
        total = jnp.zeros_like(out_ref)
        for k in range(0, own_tiles, 2):
            group = [block * own_tiles + j for j in range(k, min(k + 2, own_tiles))]
            total = total + product(group, own_all, group)
        out_ref[...] += total

    def add_term(*blocks, tiles=range(touched)):
        total = jnp.zeros_like(out_ref)
        for block, k in itertools.product(blocks, tiles[::2]):
            group = range(k, min(k + 2, tiles[-1] + 1))
            total = total + product(
                [tiles_smem[block, 0, j] for j in group],
                term_all,
                [block * touched + j for j in group],
            )
        out_ref[...] += total

    def work(stream, add, hop):
        blocks = [scen * 2 + core for core in range(2) for scen in place.origins(hop)]
        return [lambda: stream.settle(hop)] + [functools.partial(add, block) for block in blocks]

    def add_last(chunk):
        term.settle(hops, [chunk])
        last = place.origin(0, hops) * 2
        tiles = range(chunk * term.step, (chunk + 1) * term.step)
        add_term(last, last + 1, tiles=tiles)

    def run(todo, count):
        for _ in range(min(count, len(todo))):
            todo.pop(0)()

    whole_tiles = own_rows % TILE == 0
    load_border.wait()
    crossings[0].wait_recv()
    load_live.wait()
    live = jnp.clip(live_ref[0, 0], 0, 2 * half_rows)
    live_mask = lax.broadcasted_iota(jnp.int32, (2 * half_rows, half_rhs), 0) < live
    picked = jnp.concatenate(
        [
            low_all[own_tiles_ref[0, k] * per_tile + part]
            for k in range(touched)
            for part in range(per_tile)
        ],
        axis=0,
    )
    values = jnp.dot(border[...], picked, preferred_element_type=jnp.float32)
    values = jnp.where(live_mask, values, 0.0).astype(jnp.bfloat16)
    load_inverse.wait()

    def solve(start):
        rows = pl.ds(pl.multiple_of(start, half_rows), half_rows)
        rows_live = lax.broadcasted_iota(jnp.int32, (half_rows, half_rhs), 0) + start < live
        part = jnp.dot(inverse[rows], values, preferred_element_type=jnp.float32)
        return rows, jnp.where(rows_live, part, 0.0).astype(jnp.bfloat16)

    def couple(rows, part, columns):
        return lax.dot_general(
            border[rows, columns],
            part,
            (((0,), (0,)), ((), ())),
            preferred_element_type=jnp.float32,
        )

    drain(2)
    near_terms[...] = couple(*solve(side * half_rows), pl.ds(0, coupled))
    pltpu.make_async_copy(precon, precon, local_sems.at[5]).wait()
    out_ref[...] = guess[...]
    todo = work(own, add_own, 0) + work(own, add_own, 1) if whole_tiles else []
    run(todo, len(todo))
    crossings[1].wait_recv()
    far = solve((1 - side) * half_rows)
    width = term.step * TILE
    for chunk in range(term.chunks):
        columns = pl.ds(chunk * width, width)
        terms = near_terms[columns] + couple(*far, columns)
        term_all[pl.ds(own_block * touched + chunk * term.step, term.step)] = terms.astype(
            jnp.bfloat16
        ).reshape(term.step, TILE, half_rhs)
        if chunk:
            term.send([chunk - 1])
    term.send([term.chunks - 1])
    term.share()

    for hop in range(hops + 1):
        tiles.settle(hop)
    to_smem = pltpu.make_async_copy(tiles_all, tiles_smem, local_sems.at[6])
    to_smem.start()
    to_smem.wait()

    todo = []
    for hop in range(1, hops + 1):
        todo += work(term, add_term, hop - 1)
        if whole_tiles and hop < hops:
            todo = work(own, add_own, hop + 1) + todo
        rounds = term.rounds(hop)
        share = -(-len(todo) // len(rounds))
        for arrivals in rounds:
            if flow:
                own.relay(*flow.pop(0))
            term.relay(hop, arrivals)
            if flow and flow[0][0] <= hop:
                own.relay(*flow.pop(0))
            run(todo, share)
            if hop == hops and arrivals[0][2]:
                add_last(arrivals[0][2] - 1)
        drain(hop + 1)
        run(todo, len(todo))
    add_last(term.chunks - 1)
    if not whole_tiles:
        for hop in range(hops + 1):
            own.settle(hop)

        @pl.loop(0, columns_count)
        def add_column(t):
            rows = [t * per_tile + part for part in range(per_tile)]
            out_ref[...] += product([t], own_all, rows)

    drain(hops)
    for stream in (low, own, term, tiles):
        stream.finish()
    for crossing in crossings:
        crossing.wait_send()


def local(
    count,
    start_guess,
    right_side,
    root_diagonal,
    preconditioner,
    border_block,
    coupling_inverse,
    border_count,
    column_tiles,
):
    own_rows, half_rhs = start_guess.shape
    order = preconditioner.shape[1]
    half_rows, coupled = border_block.shape[1:]
    blocks = count * 2
    touched = column_tiles.shape[1]
    hops = count // 2
    ring_sems = []
    unit = math.gcd(own_rows, TILE)
    units = own_rows // unit
    for rows, step in ((units, LOW_STEP), (units, OWN_STEP), (touched, TERM_STEP), (1, 1)):
        chunks = rows // min(step, rows)
        ring_sems += [
            pltpu.SemaphoreType.DMA((1,)),
            pltpu.SemaphoreType.DMA((4 * hops * chunks,)),
            pltpu.SemaphoreType.DMA((1,)),
            pltpu.SemaphoreType.DMA((hops + chunks,)),
        ]
    vmem = pl.BlockSpec(memory_space=pltpu.VMEM)
    anywhere = pl.BlockSpec(memory_space=pltpu.HBM)
    return pl.pallas_call(
        functools.partial(kernel, count),
        out_shape=pltpu.VMEM((own_rows, half_rhs), jnp.float32),
        in_specs=[anywhere] * 8,
        out_specs=vmem,
        scratch_shapes=[
            pltpu.SMEM((1,) + border_count.shape, jnp.int32),
            pltpu.SMEM(column_tiles.shape, jnp.int32),
            pltpu.VMEM((own_rows, half_rhs), jnp.float32),
            pltpu.VMEM((own_rows, half_rhs), jnp.float32),
            pltpu.VMEM((1, own_rows), jnp.float32),
            pltpu.VMEM((order // unit, unit, half_rhs), jnp.bfloat16),
            pltpu.VMEM((order // unit, unit, half_rhs), jnp.bfloat16),
            pltpu.VMEM((blocks * touched, TILE, half_rhs), jnp.bfloat16),
            pltpu.VMEM((blocks, 1, TILE), jnp.int32),
            pltpu.SMEM((blocks, 1, TILE), jnp.int32),
            pltpu.VMEM((order // TILE, own_rows, TILE), jnp.bfloat16),
            pltpu.VMEM((2 * half_rows, coupled), jnp.bfloat16),
            pltpu.VMEM((2 * half_rows, 2 * half_rows), jnp.bfloat16),
            pltpu.VMEM((coupled, half_rhs), jnp.float32),
            pltpu.SemaphoreType.DMA((9,)),
            pltpu.SemaphoreType.DMA((2,)),
            pltpu.SemaphoreType.DMA((2,)),
        ]
        + ring_sems,
        compiler_params=pltpu.CompilerParams(
            collective_id=0, has_side_effects=True, vmem_limit_bytes=60 * 1024 * 1024
        ),
    )(
        start_guess,
        right_side,
        root_diagonal[None, :],
        preconditioner,
        border_block,
        coupling_inverse,
        border_count[None, :],
        column_tiles,
    )


def solution(mesh):
    rows = ("scen", "rootr")
    placed = (
        P(rows, "rootc"),
        P(rows, "rootc"),
        P(rows),
        P(rows, None),
        P(rows, "rootc", None),
        P(rows, "rootc", None),
        P(rows),
        P(rows, None),
    )
    return jax.shard_map(
        functools.partial(local, mesh.shape["scen"]),
        mesh=mesh,
        in_specs=placed,
        out_specs=P(rows, "rootc"),
        check_vma=False,
    )
```

```python
import functools
import itertools
import math

import jax
import jax.numpy as jnp
from jax import lax
from jax.experimental import pallas as pl
from jax.experimental.pallas import tpu as pltpu
from jax.sharding import PartitionSpec as P

TILE = 128
MESH = pl.DeviceIdType.MESH
LOW_STEP = 1
OWN_STEP = 2
TERM_STEP = 2
AHEAD = 2


class Place:
    def __init__(self, count):
        self.count, self.hops = count, count // 2
        self.scen, self.core = lax.axis_index("scen"), lax.axis_index("rootr")
        side, level = lax.rem(self.scen, 2), lax.div(self.scen, 2)
        self.spot = level * (1 - side) + (count - 1 - level) * side
        self.ahead = [self.at(1), self.at(count - 1)]

    def at(self, shift):
        spot = lax.rem(self.spot + shift, self.count)
        upper = lax.div(spot, self.hops)
        return (1 - upper) * 2 * spot + upper * (2 * (self.count - 1 - spot) + 1)

    def origin(self, way, hop):
        return self.at(self.count - hop if way == 0 else hop)

    def origins(self, hop):
        if hop == 0:
            return [self.scen]
        if hop == self.hops:
            return [self.origin(0, hop)]
        return [self.origin(0, hop), self.origin(1, hop)]


class Stream:
    def __init__(self, place, hub, buf, rows, step, sems):
        self.hub = hub
        self.place, self.buf, self.rows, self.step = place, buf, rows, step
        self.chunks = rows // step
        self.ring_send, self.ring_recv, self.pair_send, self.pair_recv = sems
        self.forwarded = self.shared = 0

    def piece(self, scen, core, chunk):
        first = (scen * 2 + core) * self.rows + chunk * self.step
        return self.buf.at[pl.ds(first, self.step)]

    def carried(self, way, hop, core):
        return hop < self.place.hops or way == core

    def rounds(self, hop):
        return [
            [
                (way, core, chunk)
                for core in (self.hub, 1 - self.hub)
                for way in range(2)
                if self.carried(way, hop, core)
            ]
            for chunk in range(self.chunks)
        ]

    def ring_copy(self, way, hop, core, chunk, ref):
        slot = ((way * self.place.hops + hop - 1) * 2 + core) * self.chunks + chunk
        return pltpu.make_async_remote_copy(
            src_ref=ref,
            dst_ref=ref,
            send_sem=self.ring_send.at[0],
            recv_sem=self.ring_recv.at[slot],
            device_id={"scen": self.place.ahead[way], "rootr": self.hub},
            device_id_type=MESH,
        )

    def pair_copy(self, hop, ref):
        return pltpu.make_async_remote_copy(
            src_ref=ref,
            dst_ref=ref,
            send_sem=self.pair_send.at[0],
            recv_sem=self.pair_recv.at[hop],
            device_id={"rootr": 1 - self.place.core},
            device_id_type=MESH,
        )

    def send(self, chunks):
        for core in range(2):

            @pl.when(self.place.core == core)
            def start():
                for chunk in chunks:
                    ref = self.piece(self.place.scen, core, chunk)
                    for way in range(2):
                        if self.carried(way, 1, core):
                            self.ring_copy(way, 1, core, chunk, ref).start()

    def share(self):
        own = self.buf.at[pl.ds((self.place.scen * 2 + self.place.core) * self.rows, self.rows)]
        self.pair_copy(0, own).start()

    def begin(self):
        self.send(range(self.chunks))
        self.share()

    def relay(self, hop, arrivals):
        for way, core, chunk in arrivals:
            self.forwarded += self.step * (hop < self.place.hops and self.carried(way, hop + 1, core))
            self.shared += self.step

        @pl.when(self.place.core == self.hub)
        def forward():
            for way, core, chunk in arrivals:
                ref = self.piece(self.place.origin(way, hop), core, chunk)
                self.ring_copy(way, hop, core, chunk, ref).wait_recv()
                if hop < self.place.hops and self.carried(way, hop + 1, core):
                    self.ring_copy(way, hop + 1, core, chunk, ref).start()
                self.pair_copy(self.pair_slot(hop, chunk), ref).start()

    def pair_slot(self, hop, chunk):
        return hop + chunk * (hop == self.place.hops)

    def settle(self, hop, chunks=None):
        if hop == 0:
            self.pair_copy(0, self.buf.at[pl.ds(0, self.rows)]).wait_recv()
            return

        @pl.when(self.place.core != self.hub)
        def arrived():
            if hop < self.place.hops:
                self.pair_copy(hop, self.buf.at[pl.ds(0, 4 * self.rows)]).wait_recv()
                return
            for chunk in range(self.chunks) if chunks is None else chunks:
                ref = self.buf.at[pl.ds(0, 2 * self.step)]
                self.pair_copy(self.pair_slot(hop, chunk), ref).wait_recv()

    def finish(self):
        for core in range(2):
            ways = sum(self.carried(way, 1, core) for way in range(2))
            ring_rows = ways * self.rows + (core == self.hub) * self.forwarded
            pair_rows = self.rows + (core == self.hub) * self.shared

            @pl.when(self.place.core == core)
            def sent():
                ref = self.buf.at[pl.ds(0, ring_rows)]
                self.ring_copy(0, 1, 0, 0, ref).wait_send()
                self.pair_copy(0, self.buf.at[pl.ds(0, pair_rows)]).wait_send()


def kernel(
    count,
    guess_hbm,
    right_hbm,
    diagonal_hbm,
    precon_hbm,
    border_hbm,
    inverse_hbm,
    live_hbm,
    own_tiles_hbm,
    out_ref,
    live_ref,
    own_tiles_ref,
    guess,
    right,
    diagonal,
    low_all,
    own_all,
    term_all,
    tiles_all,
    tiles_smem,
    precon,
    border,
    inverse,
    near_terms,
    local_sems,
    cross_send,
    cross_recv,
    *ring_sems,
):
    place = Place(count)
    hops = place.hops
    side = lax.axis_index("rootc")
    own_rows, half_rhs = guess.shape
    half_rows, coupled = border_hbm.shape[1:]
    touched = coupled // TILE
    own_block = place.scen * 2 + place.core

    barrier = pltpu.get_barrier_semaphore()
    peers = [{"scen": scen, "rootr": core} for scen in place.ahead for core in range(2)]
    peers += [{"rootr": 1 - place.core}, {"rootc": 1 - side}]
    for peer in peers:
        pl.semaphore_signal(barrier, inc=1, device_id=peer, device_id_type=MESH)

    load_guess = pltpu.make_async_copy(guess_hbm, guess, local_sems.at[0])
    load_right = pltpu.make_async_copy(right_hbm, right, local_sems.at[1])
    load_diagonal = pltpu.make_async_copy(diagonal_hbm, diagonal, local_sems.at[2])
    own_half = pl.ds(pl.multiple_of(side * half_rows, half_rows), half_rows)
    load_border = pltpu.make_async_copy(border_hbm.at[0], border.at[own_half], local_sems.at[3])
    load_inverse = pltpu.make_async_copy(inverse_hbm.at[0], inverse.at[own_half], local_sems.at[4])
    load_live = pltpu.make_async_copy(live_hbm, live_ref, local_sems.at[7])
    load_tiles = pltpu.make_async_copy(own_tiles_hbm, own_tiles_ref, local_sems.at[8])
    columns_count = precon.shape[0]
    loads = (load_guess, load_tiles, load_right, load_diagonal, load_border, load_inverse, load_live)
    for load in loads:
        load.start()

    unit = low_all.shape[1]
    units = own_rows // unit
    per_tile = TILE // unit
    own_slice = pl.ds(own_block * units, units)
    split = (units, unit, half_rhs)
    load_guess.wait()
    low_all[own_slice] = guess[...].astype(jnp.bfloat16).reshape(split)

    low = Stream(place, 1, low_all, units, min(LOW_STEP, units), ring_sems[0:4])
    own = Stream(place, 0, own_all, units, min(OWN_STEP, units), ring_sems[4:8])
    term = Stream(place, 1, term_all, touched, TERM_STEP, ring_sems[8:12])
    tiles = Stream(place, 1, tiles_all, 1, 1, ring_sems[12:16])

    pl.semaphore_wait(barrier, len(peers))
    low.begin()
    crossings = []
    for index, (source, target) in enumerate(((border_hbm, border), (inverse_hbm, inverse))):
        crossing = pltpu.make_async_remote_copy(
            src_ref=source.at[0],
            dst_ref=target.at[own_half],
            send_sem=cross_send.at[index],
            recv_sem=cross_recv.at[index],
            device_id={"rootc": 1 - side},
            device_id_type=MESH,
        )
        crossing.start()
        crossings.append(crossing)
    load_tiles.wait()
    lanes = lax.broadcasted_iota(jnp.int32, (1, 1, TILE), 2)
    tiles_row = jnp.zeros((1, 1, TILE), jnp.int32)
    for k in range(touched):
        tiles_row = jnp.where(lanes == k, own_tiles_ref[0, k], tiles_row)
    tiles_all[pl.ds(own_block, 1)] = tiles_row
    tiles.begin()

    load_right.wait()
    load_diagonal.wait()
    scale = jnp.broadcast_to(diagonal[...], (half_rhs, own_rows)).T
    own_terms = right[...] - scale * guess[...]
    own_all[own_slice] = own_terms.astype(jnp.bfloat16).reshape(split)

    @pl.loop(0, columns_count)
    def start_column(t):
        columns = pl.ds(pl.multiple_of(t * TILE, TILE), TILE)
        pltpu.make_async_copy(precon_hbm.at[:, columns], precon.at[t], local_sems.at[5]).start()

    for hop in range(1, hops + 1):
        for arrivals in low.rounds(hop):
            low.relay(hop, arrivals)
        if hop == max(hops - AHEAD, 1):
            low.settle(hop)
            own.begin()
        for arrivals in tiles.rounds(hop):
            tiles.relay(hop, arrivals)
    flow = [(hop, arrivals) for hop in range(1, hops + 1) for arrivals in own.rounds(hop)]

    def drain(stop):
        while flow and flow[0][0] <= stop:
            own.relay(*flow.pop(0))

    drain(1)
    for hop in range(hops + 1):
        if hop == hops:
            own.relay(*flow.pop(0))
        if hop != max(hops - AHEAD, 1):
            low.settle(hop)

    def product(columns, values, rows):
        left = jnp.concatenate([precon[t] for t in columns], axis=1)
        right = jnp.concatenate([values[t] for t in rows], axis=0)
        return jnp.dot(left, right, preferred_element_type=jnp.float32)

    own_tiles = own_rows // TILE

    def add_own(block):
        total = jnp.zeros_like(out_ref)
        for k in range(0, own_tiles, 2):
            group = [block * own_tiles + j for j in range(k, min(k + 2, own_tiles))]
            total = total + product(group, own_all, group)
        out_ref[...] += total

    def add_term(*blocks, tiles=range(touched)):
        total = jnp.zeros_like(out_ref)
        for block, k in itertools.product(blocks, tiles[::2]):
            group = range(k, min(k + 2, tiles[-1] + 1))
            total = total + product(
                [tiles_smem[block, 0, j] for j in group],
                term_all,
                [block * touched + j for j in group],
            )
        out_ref[...] += total

    def work(stream, add, hop):
        blocks = [scen * 2 + core for core in range(2) for scen in place.origins(hop)]
        return [lambda: stream.settle(hop)] + [functools.partial(add, block) for block in blocks]

    def add_last(chunk):
        term.settle(hops, [chunk])
        last = place.origin(0, hops) * 2
        tiles = range(chunk * term.step, (chunk + 1) * term.step)
        add_term(last, last + 1, tiles=tiles)

    def run(todo, count):
        for _ in range(min(count, len(todo))):
            todo.pop(0)()

    whole_tiles = own_rows % TILE == 0
    load_border.wait()
    crossings[0].wait_recv()
    load_live.wait()
    live = jnp.clip(live_ref[0, 0], 0, 2 * half_rows)
    live_mask = lax.broadcasted_iota(jnp.int32, (2 * half_rows, half_rhs), 0) < live
    picked = jnp.concatenate(
        [
            low_all[own_tiles_ref[0, k] * per_tile + part]
            for k in range(touched)
            for part in range(per_tile)
        ],
        axis=0,
    )
    values = jnp.dot(border[...], picked, preferred_element_type=jnp.float32)
    values = jnp.where(live_mask, values, 0.0).astype(jnp.bfloat16)
    load_inverse.wait()

    def solve(start):
        rows = pl.ds(pl.multiple_of(start, half_rows), half_rows)
        rows_live = lax.broadcasted_iota(jnp.int32, (half_rows, half_rhs), 0) + start < live
        part = jnp.dot(inverse[rows], values, preferred_element_type=jnp.float32)
        return rows, jnp.where(rows_live, part, 0.0).astype(jnp.bfloat16)

    def couple(rows, part, columns):
        return lax.dot_general(
            border[rows, columns],
            part,
            (((0,), (0,)), ((), ())),
            preferred_element_type=jnp.float32,
        )

    drain(2)
    near_terms[...] = couple(*solve(side * half_rows), pl.ds(0, coupled))
    pltpu.make_async_copy(precon, precon, local_sems.at[5]).wait()
    out_ref[...] = guess[...]
    todo = work(own, add_own, 0) + work(own, add_own, 1) if whole_tiles else []
    run(todo, len(todo))
    crossings[1].wait_recv()
    far = solve((1 - side) * half_rows)
    width = term.step * TILE
    for chunk in range(term.chunks):
        columns = pl.ds(chunk * width, width)
        terms = near_terms[columns] + couple(*far, columns)
        term_all[pl.ds(own_block * touched + chunk * term.step, term.step)] = terms.astype(
            jnp.bfloat16
        ).reshape(term.step, TILE, half_rhs)
        if chunk:
            term.send([chunk - 1])
    term.send([term.chunks - 1])
    term.share()

    for hop in range(hops + 1):
        tiles.settle(hop)
    to_smem = pltpu.make_async_copy(tiles_all, tiles_smem, local_sems.at[6])
    to_smem.start()
    to_smem.wait()

    todo = []
    for hop in range(1, hops + 1):
        todo += work(term, add_term, hop - 1)
        if whole_tiles and hop < hops:
            todo = work(own, add_own, hop + 1) + todo
        if hop == hops:
            drain(hops)
            for stream in (low, own, tiles):
                stream.finish()
            for crossing in crossings:
                crossing.wait_send()
        rounds = term.rounds(hop)
        share = -(-len(todo) // len(rounds))
        for arrivals in rounds:
            if flow:
                own.relay(*flow.pop(0))
            term.relay(hop, arrivals)
            if flow and flow[0][0] <= hop:
                own.relay(*flow.pop(0))
            run(todo, share)
            if hop == hops and arrivals[0][2]:
                add_last(arrivals[0][2] - 1)
        drain(hop + 1)
        run(todo, len(todo))
    add_last(term.chunks - 1)
    if not whole_tiles:
        for hop in range(hops + 1):
            own.settle(hop)

        @pl.loop(0, columns_count)
        def add_column(t):
            rows = [t * per_tile + part for part in range(per_tile)]
            out_ref[...] += product([t], own_all, rows)

    term.finish()


def local(
    count,
    start_guess,
    right_side,
    root_diagonal,
    preconditioner,
    border_block,
    coupling_inverse,
    border_count,
    column_tiles,
):
    own_rows, half_rhs = start_guess.shape
    order = preconditioner.shape[1]
    half_rows, coupled = border_block.shape[1:]
    blocks = count * 2
    touched = column_tiles.shape[1]
    hops = count // 2
    ring_sems = []
    unit = math.gcd(own_rows, TILE)
    units = own_rows // unit
    for rows, step in ((units, LOW_STEP), (units, OWN_STEP), (touched, TERM_STEP), (1, 1)):
        chunks = rows // min(step, rows)
        ring_sems += [
            pltpu.SemaphoreType.DMA((1,)),
            pltpu.SemaphoreType.DMA((4 * hops * chunks,)),
            pltpu.SemaphoreType.DMA((1,)),
            pltpu.SemaphoreType.DMA((hops + chunks,)),
        ]
    vmem = pl.BlockSpec(memory_space=pltpu.VMEM)
    anywhere = pl.BlockSpec(memory_space=pltpu.HBM)
    return pl.pallas_call(
        functools.partial(kernel, count),
        out_shape=pltpu.VMEM((own_rows, half_rhs), jnp.float32),
        in_specs=[anywhere] * 8,
        out_specs=vmem,
        scratch_shapes=[
            pltpu.SMEM((1,) + border_count.shape, jnp.int32),
            pltpu.SMEM(column_tiles.shape, jnp.int32),
            pltpu.VMEM((own_rows, half_rhs), jnp.float32),
            pltpu.VMEM((own_rows, half_rhs), jnp.float32),
            pltpu.VMEM((1, own_rows), jnp.float32),
            pltpu.VMEM((order // unit, unit, half_rhs), jnp.bfloat16),
            pltpu.VMEM((order // unit, unit, half_rhs), jnp.bfloat16),
            pltpu.VMEM((blocks * touched, TILE, half_rhs), jnp.bfloat16),
            pltpu.VMEM((blocks, 1, TILE), jnp.int32),
            pltpu.SMEM((blocks, 1, TILE), jnp.int32),
            pltpu.VMEM((order // TILE, own_rows, TILE), jnp.bfloat16),
            pltpu.VMEM((2 * half_rows, coupled), jnp.bfloat16),
            pltpu.VMEM((2 * half_rows, 2 * half_rows), jnp.bfloat16),
            pltpu.VMEM((coupled, half_rhs), jnp.float32),
            pltpu.SemaphoreType.DMA((9,)),
            pltpu.SemaphoreType.DMA((2,)),
            pltpu.SemaphoreType.DMA((2,)),
        ]
        + ring_sems,
        compiler_params=pltpu.CompilerParams(
            collective_id=0, has_side_effects=True, vmem_limit_bytes=60 * 1024 * 1024
        ),
    )(
        start_guess,
        right_side,
        root_diagonal[None, :],
        preconditioner,
        border_block,
        coupling_inverse,
        border_count[None, :],
        column_tiles,
    )


def solution(mesh):
    rows = ("scen", "rootr")
    placed = (
        P(rows, "rootc"),
        P(rows, "rootc"),
        P(rows),
        P(rows, None),
        P(rows, "rootc", None),
        P(rows, "rootc", None),
        P(rows),
        P(rows, None),
    )
    return jax.shard_map(
        functools.partial(local, mesh.shape["scen"]),
        mesh=mesh,
        in_specs=placed,
        out_specs=P(rows, "rootc"),
        check_vma=False,
    )
```
